32 devices in a mesh: tm: 4 (over z), paths: 8 (over y, x, core).
Axes of the slice: x: 2, y: 2, z: 4, core: 2. Of those that a mesh axis runs over, the one named last changes fastest.
Arguments:
- start_curve: float32 [80], replicated, may hold values from 0.02 to 0.06
- loadings: float32 [4, 80], replicated, may hold values from 0.2 to 1
- vols: float32 [40, 80], P('tm'), may hold values from 0.08 to 0.4
- shocks: float32 [40, 4, 16384], P('tm', None, 'paths'), may hold values from -5 to 5
- exercise_bits: int32 [40, 16384], P('tm', 'paths'), may hold values 0 or 1
- regress: float32 [40, 6], P('tm'), may hold values from -0.03 to 0.03
- date_slot: int32 [40], P('tm'), may hold values from 0 to 39, each once
- ck_rates: float32 [4, 80, 16384], P('tm', None, 'paths'), may hold values from 0.02 to 0.07
- ck_numer: float32 [4, 16384], P('tm', 'paths'), may hold values from 1 to 3
- ck_survive: float32 [4, 16384], P('tm', 'paths'), may hold values from 0.2 to 1
Outputs:
- vega: float32 [40, 80], P('tm')
- path_value: float32 [16384], P('paths')
The draws below stay inside these ranges and needn't reach their ends.
Inputs may be any that keep to these rules, and one draw needn't show every extreme that they name: `date_slot`: each row of regress is named once: a permutation of the 40 rows.
All inputs are finite; a program needn't handle non-finite values. No bound on the sum of `exercise_bits` on one device may be relied on, other than what follows from the above.
Results may differ from the reference program's by a relative error of at most 0.0003.
Values sent between devices are 32-bit elements; how exact they have to be, the bound alone decides.
No kernel may reach another device: no remote copies, remote signals or barrier semaphores. Data moves between devices by JAX's collectives and lax.ppermute only.
A program may use at most 128 MiB of HBM per device.

```python
import math
import jax
import jax.numpy as jnp
from jax import lax

NF = 80
NE = 40
FACTORS = 4
BASIS = 6
PATHS = 16384
SHARDS = 4
N_TM = 4
N_PATHS = 8


def plant(result, key, low, top_value):
    dims = result.shape
    place = [jax.random.randint(jax.random.fold_in(key, axis), (), 0, dims[axis]) for axis in range(len(dims))]
    result = result.at[tuple(place)].set(low)
    longest = dims.index(max(dims))
    place[longest] = (place[longest] + 1) % dims[longest]
    return result.at[tuple(place)].set(top_value)


def block_scale(key, extent, split, smallest, high):
    def one(axis_at, parts):
        heights = jax.random.uniform(jax.random.fold_in(jax.random.fold_in(key, 6), axis_at), (parts,), jnp.float32, smallest / len(split), high / len(split))
        return jnp.repeat(jnp.exp(heights), extent[axis_at] // parts).reshape((-1,) + (1,) * (len(extent) - axis_at - 1))

    factor_of = one(*split[0])
    for cut in split[1:]:
        factor_of = factor_of * one(*cut)
    return factor_of


def bell_draw(rng, extent, deviation, most, pieces=(), kind=jnp.bfloat16):
    drawn = jax.random.normal(rng, extent, jnp.float32) * deviation
    if len(pieces) > 0:
        drawn = block_scale(rng, extent, pieces, -0.22, 0.18) * drawn
    return jnp.clip(drawn, min=-most, max=most).astype(kind)


def setup_inputs(seed: int = 0) -> dict:
    splits = jax.random.split(jax.random.key(seed), 11)
    start_curve = jnp.clip(jax.random.uniform(splits[0], (NF,), jnp.float32, 0.02, 0.06), 0.02, 0.06)
    loadings = jnp.clip(jax.random.uniform(splits[1], (FACTORS, NF), jnp.float32, 0.2, 1.0), 0.2, 1.0)
    vols = jnp.clip(jnp.exp(math.log(0.4) - 1.609438 * jax.random.uniform(splits[2], (NE, NF), jnp.float32) ** block_scale(splits[2], (NE, NF), ((0, 4),), -0.2, 0.2)), 0.08, 0.4)
    shocks = bell_draw(splits[3], (NE, FACTORS, PATHS), 1.0, 5.0, ((0, 4), (2, 8)), jnp.float32)
    exercise_bits = plant((jax.random.randint(splits[4], (NE, PATHS), 0, 2) < 1).astype(jnp.int32), jax.random.fold_in(splits[4], 1), 0, 1)
    regress = bell_draw(splits[5], (NE, BASIS), 0.005, 0.03, ((0, 4),), jnp.float32)
    date_slot = jax.random.permutation(splits[6], NE).astype(jnp.int32)
    ck_rates = jnp.clip(0.02 + 0.05 * jax.random.uniform(splits[7], (SHARDS, NF, PATHS), jnp.float32) ** block_scale(splits[7], (SHARDS, NF, PATHS), ((0, 4), (2, 8)), -0.2, 0.2), 0.02, 0.07)
    ck_numer = jnp.clip(1.0 + 2.0 * jax.random.uniform(splits[8], (SHARDS, PATHS), jnp.float32) ** block_scale(splits[8], (SHARDS, PATHS), ((0, 4), (1, 8)), -0.2, 0.2), 1.0, 3.0)
    ck_survive = jnp.clip(0.2 + 0.8 * jax.random.uniform(splits[9], (SHARDS, PATHS), jnp.float32) ** block_scale(splits[9], (SHARDS, PATHS), ((0, 4), (1, 8)), -0.2, 0.2), 0.2, 1.0)
    return dict(start_curve=start_curve, loadings=loadings, vols=vols, shocks=shocks, exercise_bits=exercise_bits, regress=regress, date_slot=date_slot, ck_rates=ck_rates, ck_numer=ck_numer, ck_survive=ck_survive)


ACCRUAL = 0.25
STRIKE = 0.04
SMOOTHING = 0.01
NOTIONAL = 100.0
HIGHEST = lax.Precision.HIGHEST

def segment(rates_in, numeraire, survival, vol_rows, shock_rows, flag_rows, weight_rows, loadings, first_date):
    forwards = rates_in.shape[0]
    positions = jnp.arange(forwards, dtype=jnp.int32)
    triangle = (positions[:, None] >= positions[None, :]).astype(jnp.float32)
    factor_loads = loadings / jnp.sqrt(lax.optimization_barrier(jnp.sum(loadings * loadings, axis=0, keepdims=True)))
    current = rates_in
    path_total = jnp.zeros(numeraire.shape, jnp.float32)
    for offset_date in range(vol_rows.shape[0]):
        date_index = first_date + offset_date
        opening = 2 * date_index + 1
        earlier = jnp.where(date_index == 0, 0, 2 * date_index - 1)
        horizon = jnp.where(date_index == 0, ACCRUAL, 2.0 * ACCRUAL)
        growth = jnp.log1p(ACCRUAL * current)
        fixing = ((positions >= earlier) & (positions < opening)).astype(jnp.float32)
        numeraire = numeraire * jnp.exp(lax.optimization_barrier(jnp.sum(fixing[:, None] * growth, axis=0)))
        living = (positions >= opening).astype(jnp.float32)
        sigma = vol_rows[offset_date] * living
        scaled = ACCRUAL * current * sigma[:, None] / (1.0 + ACCRUAL * current)
        running = jnp.einsum('ij,fjp->fip', triangle, factor_loads[:, :, None] * scaled[None], precision=HIGHEST)
        drift = sigma[:, None] * lax.optimization_barrier(jnp.sum(factor_loads[:, :, None] * running, axis=0))
        noise = jnp.einsum('fi,fp->ip', factor_loads, shock_rows[offset_date], precision=HIGHEST)
        exponent = horizon * drift - 0.5 * horizon * (sigma * sigma)[:, None] + jnp.sqrt(horizon) * sigma[:, None] * noise
        current = current * jnp.exp(exponent)
        discount = jnp.dot(triangle, living[:, None] * jnp.log1p(ACCRUAL * current), precision=HIGHEST)
        bonds = jnp.exp(-discount)
        annuity = ACCRUAL * lax.optimization_barrier(jnp.sum(living[:, None] * bonds, axis=0))
        floating = 1.0 - bonds[forwards - 1]
        exercise = floating - STRIKE * annuity
        moneyness = (floating / annuity - STRIKE) / SMOOTHING
        basis = jnp.stack([jnp.ones_like(moneyness), moneyness, moneyness * moneyness, annuity, annuity * moneyness, annuity * moneyness * moneyness])
        continuation = jnp.einsum('b,bp->p', weight_rows[offset_date], basis, precision=HIGHEST)
        chance = flag_rows[offset_date] * jax.nn.sigmoid((exercise - continuation) / SMOOTHING)
        path_total = path_total + NOTIONAL * survival * chance * exercise / numeraire
        survival = survival * (1.0 - chance)
    return (current, numeraire, survival, path_total)

def chained(every_vols, every_weights, shock_block, flag_block, rate_block, numer_block, survive_block, start_curve, loadings, per_shard, shard_count):
    width_paths = shock_block.shape[2]
    current = jnp.broadcast_to(start_curve[:, None], (start_curve.shape[0], width_paths))
    numeraire = jnp.ones((width_paths,), jnp.float32)
    survival = jnp.ones((width_paths,), jnp.float32)
    running_total = jnp.zeros((width_paths,), jnp.float32)
    for shard_index in range(shard_count):
        if shard_index > 0:
            current = rate_block[shard_index - 1] + (current - lax.stop_gradient(current))
            numeraire = numer_block[shard_index - 1] + (numeraire - lax.stop_gradient(numeraire))
            survival = survive_block[shard_index - 1] + (survival - lax.stop_gradient(survival))
        first_row = shard_index * per_shard
        last_row = first_row + per_shard
        current, numeraire, survival, segment_value = segment(current, numeraire, survival, every_vols[first_row:last_row], shock_block[first_row:last_row], flag_block[first_row:last_row], every_weights[first_row:last_row], loadings, first_row)
        running_total = running_total + segment_value
    return running_total

def reference(start_curve, loadings, vols, shocks, exercise_bits, regress, date_slot, ck_rates, ck_numer, ck_survive):
    per_shard = NE // N_TM
    per_group = PATHS // N_PATHS
    date_weights = regress[date_slot]
    flag_rows = exercise_bits.astype(jnp.float32)

    def one_group(vega_total, group_index):
        first_path = (group_index * per_group).astype(jnp.int32)

        def cut_paths(array_in, axis_number):
            return lax.dynamic_slice_in_dim(array_in, first_path, per_group, axis_number)
        shock_block = cut_paths(shocks, 2)
        flag_block = cut_paths(flag_rows, 1)
        rate_block = cut_paths(ck_rates, 2)
        numer_block = cut_paths(ck_numer, 1)
        survive_block = cut_paths(ck_survive, 1)

        def runner(every_vols):
            return chained(every_vols, date_weights, shock_block, flag_block, rate_block, numer_block, survive_block, start_curve, loadings, per_shard, N_TM)
        values, reverse_map = jax.vjp(runner, vols)
        gradient = reverse_map(jnp.full_like(values, NOTIONAL / PATHS))[0]
        return (vega_total + gradient, values)
    vega, values = lax.scan(one_group, jnp.zeros_like(vols), jnp.arange(N_PATHS, dtype=jnp.int32))
    return (vega, values.reshape(PATHS))
```

```python
import functools

import jax
import jax.numpy as jnp
from jax import lax
from jax.experimental import pallas as pl
from jax.experimental.pallas import tpu as pltpu
from jax.sharding import PartitionSpec as P

ACCRUAL = 0.25
STRIKE = 0.04
SMOOTHING = 0.01
NOTIONAL = 100.0
LANES = 128
BLOCK = 8


def kernel(
    place_ref,
    vol_ref,
    ratio_ref,
    regress_ref,
    slot_ref,
    curve_ref,
    *refs,
    shards,
    per_shard,
    forwards,
    factors,
    basis,
    low_row,
):
    block_refs = refs[:shards]
    vega_ref, value_ref = refs[shards : shards + 2]
    (
        inbox,
        rate,
        disc,
        res_growth,
        res_exp,
        res_slope,
        res_tilt,
        res_drive,
        res_disc,
        res_sum,
        grads,
        annuities,
        finals,
        numers,
        fixes,
        seeds_a,
        seeds_b,
        numer_adj,
        survs,
        chances,
        pays,
        adjoint,
        arrived,
    ) = refs[shards + 2 :]
    dates = shards * per_shard
    blocks = forwards // BLOCK
    sub = value_ref.shape[0]
    tile = (sub, LANES)
    place = place_ref[0]
    row_flag = per_shard * factors
    row_rates = row_flag + per_shard
    row_numer = row_rates + forwards - low_row
    row_survive = row_numer + 1

    def fetch(step):
        source = lax.rem(place - step + shards, shards)
        return pltpu.make_async_copy(block_refs[step], inbox.at[source], arrived.at[step])

    for step in range(shards):
        fetch(step).start()
    for step in range(shards):
        fetch(step).wait()

    def first_block(opening):
        return opening // BLOCK

    def forward_date(shard, offset, carry):
        pos, numer = carry
        date = shard * per_shard + offset
        opening = 2 * date + 1
        is_start = date == 0
        horizon = jnp.where(is_start, ACCRUAL, 2.0 * ACCRUAL)
        inv_root = jnp.where(is_start, ACCRUAL**-0.5, (2.0 * ACCRUAL) ** -0.5)
        near = jnp.maximum(opening - 2, 0)
        last = opening - 1
        numer = numer * (1.0 + rate[last])
        numer = numer * jnp.where(is_start, 1.0, 1.0 + rate[near])
        numers[date] = numer
        fixes[2 * date] = disc[near]
        fixes[2 * date + 1] = disc[last]
        sums = tuple(inbox[shard, offset * factors + f] * inv_root for f in range(factors))

        def one_block(block, state, masked):
            pos, sums, bond, total = state
            sums = list(sums)
            for inner in range(BLOCK):
                row = block * BLOCK + inner
                at = pos * BLOCK + inner
                vol = vol_ref[date * forwards + row]
                if masked:
                    alive = row >= opening
                    vol = jnp.where(alive, vol, 0.0)
                lead = vol * ratio_ref[row]
                half = vol * ratio_ref[forwards + row]
                timed = horizon * lead
                old = disc[row]
                drive = lead * (1.0 - old)
                sums[0] = sums[0] + drive
                tilt = sums[0]
                for f in range(1, factors):
                    scale = ratio_ref[(f + 1) * forwards + row]
                    sums[f] = sums[f] + scale * drive
                    tilt = tilt + scale * sums[f]
                tilt = tilt - half
                grow = jnp.exp(timed * tilt)
                new = rate[row] * grow
                fresh = 1.0 / (1.0 + new)
                rate[row] = new
                disc[row] = fresh
                res_growth[at] = timed * new
                res_exp[at] = grow
                res_slope[at] = lead * (old * old)
                res_tilt[at] = tilt - half
                res_drive[at] = drive
                res_sum[at] = total
                if masked:
                    mask = alive.astype(jnp.float32)
                    res_disc[at] = fresh * mask
                    bond = bond * jnp.where(alive, fresh, 1.0)
                    total = total + bond * mask
                else:
                    res_disc[at] = fresh
                    bond = bond * fresh
                    total = total + bond
            return (pos + 1, tuple(sums), bond, total)

        begin = first_block(opening)
        state = one_block(
            begin, (pos, sums, jnp.ones(tile, jnp.float32), jnp.zeros(tile, jnp.float32)), True
        )
        pos, _, bond, total = lax.fori_loop(
            begin + 1, blocks, lambda block, s: one_block(block, s, False), state
        )
        annuities[date] = ACCRUAL * total
        finals[date] = bond
        return (pos, numer)

    pos = jnp.int32(0)
    ends = []
    for shard in range(shards):
        if shard == 0:
            def fill(row, _):
                start = jnp.full(tile, ACCRUAL * curve_ref[row], jnp.float32)
                rate[row] = start
                disc[row] = 1.0 / (1.0 + start)
                return 0

            lax.fori_loop(0, forwards, fill, 0, unroll=BLOCK)
            numer = jnp.ones(tile, jnp.float32)
        else:
            lowest = (2 * shard * per_shard - 1) // BLOCK * BLOCK

            def fill(row, _, shard=shard):
                start = ACCRUAL * inbox[shard - 1, row_rates + row - low_row]
                rate[row] = start
                disc[row] = 1.0 / (1.0 + start)
                return 0

            lax.fori_loop(lowest, forwards, fill, 0, unroll=BLOCK)
            numer = inbox[shard - 1, row_numer]
        pos, numer = lax.fori_loop(
            0, per_shard, functools.partial(forward_date, shard), (pos, numer)
        )
        ends.append(numer)

    value = jnp.zeros(tile, jnp.float32)
    for shard in range(shards):
        if shard == 0:
            survive = jnp.ones(tile, jnp.float32)
        else:
            survive = inbox[shard - 1, row_survive]

        def stage(offset, carry, shard=shard):
            survive, value = carry
            date = shard * per_shard + offset
            annuity = annuities[date]
            floating = 1.0 - finals[date]
            slot = slot_ref[date] * basis
            w = [regress_ref[slot + q] for q in range(basis)]
            inverse = 1.0 / annuity
            swap = floating * inverse
            money = (swap - STRIKE) * (1.0 / SMOOTHING)
            exercise = floating - STRIKE * annuity
            inner = w[3] + money * (w[4] + money * w[5])
            continuation = w[0] + money * (w[1] + money * w[2]) + annuity * inner
            sigmoid = jax.nn.sigmoid((exercise - continuation) * (1.0 / SMOOTHING))
            flag = inbox[shard, row_flag + offset]
            chance = flag * sigmoid
            pay = NOTIONAL * exercise / numers[date]
            slope = chance * (1.0 - sigmoid) * (1.0 / SMOOTHING)
            money_adj = (
                w[1] + 2.0 * (w[2] * money) + annuity * (w[4] + 2.0 * (w[5] * money))
            ) * (1.0 / SMOOTHING)
            tilt_money = money_adj * inverse
            seeds_a[2 * date] = slope * (-STRIKE - inner + tilt_money * swap)
            seeds_a[2 * date + 1] = slope * (1.0 - tilt_money)
            chances[date] = chance
            pays[date] = pay
            survs[date] = survive
            value = value + survive * chance * pay
            return (survive * (1.0 - chance), value)

        survive, value = lax.fori_loop(0, per_shard, stage, (survive, value), unroll=5)
    value_ref[...] = value

    gain_adj = jnp.zeros(tile, jnp.float32)
    log_adj = jnp.zeros(tile, jnp.float32)
    for shard in reversed(range(shards)):

        def unwind(step, carry, shard=shard):
            late, log_adj = carry
            date = shard * per_shard + per_shard - 1 - step
            chance = chances[date]
            pay = pays[date]
            survive = survs[date]
            chance_adj = survive * (pay - late)
            direct = (NOTIONAL * survive) * chance / numers[date]
            annuity_adj = chance_adj * seeds_a[2 * date] - STRIKE * direct
            float_adj = chance_adj * seeds_a[2 * date + 1] + direct
            seeds_b[2 * date] = annuity_adj * annuities[date] - float_adj * finals[date]
            seeds_b[2 * date + 1] = ACCRUAL * annuity_adj
            gain = chance * pay
            log_adj = log_adj - survive * gain
            numer_adj[date] = log_adj
            return (gain + late * (1.0 - chance), log_adj)

        gain_adj, log_adj = lax.fori_loop(0, per_shard, unwind, (gain_adj, log_adj), unroll=5)
        if shard > 0:
            log_adj = log_adj * ends[shard - 1] / inbox[shard - 1, row_numer]

    def clear(row, _):
        adjoint[row] = jnp.zeros(tile, jnp.float32)
        return 0

    lax.fori_loop(0, forwards, clear, 0, unroll=BLOCK)

    def backward_date(step, pos):
        date = dates - 1 - step
        opening = 2 * date + 1
        seed_level = seeds_b[2 * date]
        seed_slope = seeds_b[2 * date + 1]

        def one_block(back, state):
            pos, sums = state
            sums = list(sums)
            block = blocks - 1 - back
            pos = pos - 1
            for inner in reversed(range(BLOCK)):
                row = block * BLOCK + inner
                at = pos * BLOCK + inner
                pull = (seed_level - seed_slope * res_sum[at]) * res_disc[at]
                inward = adjoint[row] - pull
                timed = inward * res_growth[at]
                sums[0] = sums[0] + timed
                drive_adj = sums[0]
                for f in range(1, factors):
                    scale = ratio_ref[(f + 1) * forwards + row]
                    sums[f] = sums[f] + scale * timed
                    drive_adj = drive_adj + scale * sums[f]
                adjoint[row] = inward * res_exp[at] + drive_adj * res_slope[at]
                grads[date * forwards + row] = timed * res_tilt[at] + drive_adj * res_drive[at]
            return (pos, tuple(sums))

        zero = jnp.zeros(tile, jnp.float32)
        pos, _ = lax.fori_loop(
            0, blocks - first_block(opening), one_block, (pos, (zero,) * factors)
        )
        near = jnp.maximum(opening - 2, 0)
        last = opening - 1
        level = numer_adj[date]
        adjoint[near] = level * fixes[2 * date]
        adjoint[last] = level * fixes[2 * date + 1]
        return pos

    lax.fori_loop(0, dates, backward_date, pos)

    ones = jnp.ones((BLOCK, LANES), jnp.float32)

    def collect(date, _):
        picked = grads[pl.ds(date * forwards, forwards)]
        summed = jnp.sum(picked, axis=1)
        row = lax.dot_general(
            ones, summed, (((1,), (1,)), ((), ())),
            precision=lax.Precision.HIGHEST, preferred_element_type=jnp.float32,
        )
        vega_ref[date] = row[0:1]
        return 0

    lax.fori_loop(0, dates, collect, 0)


def turned(parts, start):
    doubled = jnp.concatenate(parts + parts, axis=0)
    return lax.dynamic_slice_in_dim(doubled, start * parts[0].shape[0], len(parts) * parts[0].shape[0], 0)


def by_source(own, received, place):
    count = len(received) + 1
    return turned([own] + received[::-1], lax.rem(count - place, count))


def exchange(blocks, axis, place):
    count = lax.axis_size(axis)
    own = lax.dynamic_index_in_dim(blocks, place, 0, keepdims=False)
    received = []
    for step in range(1, count):
        sent = lax.dynamic_index_in_dim(blocks, lax.rem(place + step, count), 0, keepdims=False)
        received.append(
            lax.ppermute(sent, axis, [(s, (s + step) % count) for s in range(count)])
        )
    return own, received


def total_over(value, axis):
    count = lax.axis_size(axis)
    if count & (count - 1):
        return lax.psum(value, axis)
    step = 1
    while step < count:
        value = value + lax.ppermute(value, axis, [(s, s ^ step) for s in range(count)])
        step *= 2
    return value


def local(
    start_curve,
    loadings,
    vols,
    shocks,
    exercise_bits,
    regress,
    date_slot,
    ck_rates,
    ck_numer,
    ck_survive,
):
    shards = lax.axis_size("tm")
    groups = lax.axis_size("paths")
    place = lax.axis_index("tm")
    per_shard, forwards = vols.shape
    factors, paths = shocks.shape[1:]
    basis = regress.shape[1]
    dates = shards * per_shard
    per_device = paths // shards
    sub = per_device // LANES
    unit = sub * LANES
    low_row = max(0, (2 * per_shard - 1) // BLOCK * BLOCK)

    def blocked(rows):
        return rows.reshape(-1, shards, sub, LANES).transpose(1, 0, 2, 3)

    small = jnp.concatenate(
        [vols.reshape(-1), regress.reshape(-1), date_slot.astype(jnp.float32)]
    )
    small_rows = -(-small.shape[0] // unit)
    small = jnp.pad(small, (0, small_rows * unit - small.shape[0]))
    payload = jnp.concatenate(
        [
            blocked(shocks.reshape(per_shard * factors, paths)),
            blocked(exercise_bits.astype(jnp.float32)),
            blocked(ck_rates[0, low_row:]),
            blocked(ck_numer),
            blocked(ck_survive),
            jnp.broadcast_to(small.reshape(1, small_rows, sub, LANES), (shards, small_rows, sub, LANES)),
        ],
        axis=1,
    )
    rows = payload.shape[1]
    own, received = exchange(payload, "tm", place)
    smalls = by_source(
        own[rows - small_rows :].reshape(1, -1),
        [part[rows - small_rows :].reshape(1, -1) for part in received],
        place,
    )
    cut = per_shard * forwards
    vol_all = smalls[:, :cut].reshape(-1)
    regress_all = smalls[:, cut : cut + per_shard * basis].reshape(-1)
    slot_all = (
        smalls[:, cut + per_shard * basis : cut + per_shard * (basis + 1)]
        .reshape(-1)
        .astype(jnp.int32)
    )
    loads = loadings / jnp.sqrt(jnp.sum(loadings * loadings, axis=0, keepdims=True))
    ratios = jnp.concatenate([loads[0], 0.5 / loads[0], (loads[1:] / loads[:1]).reshape(-1)])

    triangle = sum(
        forwards // BLOCK - min((2 * d + 1) // BLOCK, forwards // BLOCK - 1) for d in range(dates)
    )
    tile = (sub, LANES)
    f32 = jnp.float32
    residual = pltpu.VMEM((triangle * BLOCK,) + tile, f32)
    per_date = pltpu.VMEM((dates,) + tile, f32)
    two_per_date = pltpu.VMEM((2 * dates,) + tile, f32)
    per_forward = pltpu.VMEM((forwards,) + tile, f32)
    smem = pl.BlockSpec(memory_space=pltpu.SMEM)
    vega_part, value_part = pl.pallas_call(
        functools.partial(
            kernel,
            shards=shards,
            per_shard=per_shard,
            forwards=forwards,
            factors=factors,
            basis=basis,
            low_row=low_row,
        ),
        out_shape=(
            jax.ShapeDtypeStruct((dates, 1, forwards), f32),
            jax.ShapeDtypeStruct(tile, f32),
        ),
        in_specs=[smem] * 6 + [pl.BlockSpec(memory_space=pl.ANY)] * shards,
        out_specs=(
            pl.BlockSpec(memory_space=pltpu.VMEM),
            pl.BlockSpec(memory_space=pltpu.VMEM),
        ),
        scratch_shapes=[
            pltpu.VMEM((shards, rows) + tile, f32),
            per_forward,
            per_forward,
            residual,
            residual,
            residual,
            residual,
            residual,
            residual,
            residual,
            pltpu.VMEM((dates * forwards,) + tile, f32),
            per_date,
            per_date,
            per_date,
            two_per_date,
            two_per_date,
            two_per_date,
            per_date,
            per_date,
            per_date,
            per_date,
            per_forward,
            pltpu.SemaphoreType.DMA((shards,)),
        ],
        compiler_params=pltpu.CompilerParams(vmem_limit_bytes=56 * 1024 * 1024),
        name="sweep",
    )(
        place.reshape(1).astype(jnp.int32),
        vol_all,
        ratios,
        regress_all,
        slot_all,
        start_curve,
        own,
        *received,
    )

    parts = vega_part.reshape(shards, cut)
    tail = value_part.reshape(1, per_device)
    message = jnp.concatenate([parts, jnp.broadcast_to(tail, (shards, per_device))], axis=1)
    mine, others = exchange(message, "tm", place)
    path_value = by_source(
        mine[cut:].reshape(1, -1), [part[cut:].reshape(1, -1) for part in others], place
    ).reshape(-1)
    summed = mine[:cut]
    for part in others:
        summed = summed + part[:cut]
    summed = total_over(summed.reshape(per_shard, forwards), "paths")
    date = place * per_shard + jnp.arange(per_shard, dtype=jnp.int32)
    alive = jnp.arange(forwards, dtype=jnp.int32)[None, :] >= 2 * date[:, None] + 1
    weight = NOTIONAL / (paths * groups)
    vega = jnp.where(alive, summed * (weight / vols), 0.0)
    return (vega, path_value)


def solution(mesh):
    return jax.shard_map(
        local,
        mesh=mesh,
        in_specs=(
            P(),
            P(),
            P("tm", None),
            P("tm", None, "paths"),
            P("tm", "paths"),
            P("tm", None),
            P("tm"),
            P("tm", None, "paths"),
            P("tm", "paths"),
            P("tm", "paths"),
        ),
        out_specs=(P("tm", None), P("paths")),
        check_vma=False,
    )
```

```python
import functools

import jax
import jax.numpy as jnp
from jax import lax
from jax.experimental import pallas as pl
from jax.experimental.pallas import tpu as pltpu
from jax.sharding import PartitionSpec as P

ACCRUAL = 0.25
STRIKE = 0.04
SMOOTHING = 0.01
NOTIONAL = 100.0
LANES = 128
BLOCK = 16
LOG2E = 1.4426950408889634


def kernel(
    place_ref,
    vol_ref,
    ratio_ref,
    regress_ref,
    slot_ref,
    curve_ref,
    scale_ref,
    *refs,
    shards,
    per_shard,
    forwards,
    factors,
    basis,
    low_row,
):
    block_refs = refs[:shards]
    vega_ref, value_ref = refs[shards : shards + 2]
    (
        inbox,
        rate,
        res_disc,
        res_tilt,
        res_sum,
        grads,
        annuities,
        finals,
        numers,
        fixes,
        seeds_a,
        seeds_b,
        numer_adj,
        survs,
        chances,
        pays,
        adjoint,
        arrived,
    ) = refs[shards + 2 :]
    dates = shards * per_shard
    blocks = forwards // BLOCK
    sub = value_ref.shape[0]
    tile = (sub, LANES)
    place = place_ref[0]
    row_flag = per_shard * factors
    row_rates = row_flag + per_shard
    row_numer = row_rates + forwards - low_row
    row_survive = row_numer + 1
    lowest = [max(0, 2 * s * per_shard - 1) // BLOCK for s in range(shards)]

    def fetch(step):
        source = lax.rem(place - step + shards, shards)
        return pltpu.make_async_copy(block_refs[step], inbox.at[source], arrived.at[step])

    for step in range(shards):
        fetch(step).start()
    for step in range(shards):
        fetch(step).wait()

    def horizon_of(date):
        return jnp.where(date == 0, ACCRUAL, 2.0 * ACCRUAL)

    def forward_date(shard, offset, carry):
        pos, numer = carry
        date = shard * per_shard + offset
        opening = 2 * date + 1
        is_start = date == 0
        horizon = horizon_of(date)
        inv_root = jnp.where(is_start, ACCRUAL**-0.5, (2.0 * ACCRUAL) ** -0.5)
        near = jnp.maximum(opening - 2, 0)
        last = opening - 1
        before = pos - blocks
        numer = numer * (1.0 + rate[shard, last])
        numer = numer * jnp.where(is_start, 1.0, 1.0 + rate[shard, near])
        numers[date] = numer
        fixes[2 * date] = 1.0 - res_disc[before * BLOCK + near]
        fixes[2 * date + 1] = 1.0 - res_disc[before * BLOCK + last]
        sums = tuple(inbox[shard, offset * factors + f] * inv_root for f in range(factors))
        begin = opening // BLOCK
        shift = pos - begin

        def one_block(block, state, masked):
            sums, bond, total = state
            sums = list(sums)
            olds = [res_disc[(before + block) * BLOCK + inner] for inner in range(BLOCK)]
            rates = [rate[shard, block * BLOCK + inner] for inner in range(BLOCK)]
            kept = []
            for inner in range(BLOCK):
                row = block * BLOCK + inner
                vol = vol_ref[date * forwards + row]
                if masked:
                    alive = row >= opening
                    vol = jnp.where(alive, vol, 0.0)
                lead = vol * ratio_ref[row]
                half = vol * ratio_ref[forwards + row]
                timed = (horizon * LOG2E) * lead
                drive = lead * (1.0 - olds[inner])
                sums[0] = sums[0] + drive
                tilt = sums[0]
                for f in range(1, factors):
                    scale = scale_ref[(f - 1) * forwards + row]
                    sums[f] = sums[f] + scale * drive
                    tilt = tilt + scale * sums[f]
                tilt = tilt - half
                new = rates[inner] * jnp.exp2(timed * tilt)
                fresh = 1.0 / (1.0 + new)
                if masked:
                    fresh = jnp.where(alive, fresh, 1.0)
                kept.append((new, fresh, tilt - half, total))
                bond = bond * fresh
                total = total + (jnp.where(alive, bond, 0.0) if masked else bond)
            for inner, (new, fresh, lean, total_before) in enumerate(kept):
                at = (shift + block) * BLOCK + inner
                rate[shard, block * BLOCK + inner] = new
                res_disc[at] = fresh
                res_tilt[at] = lean
                res_sum[at] = total_before
            return (tuple(sums), bond, total)

        state = one_block(
            begin, (sums, jnp.ones(tile, jnp.float32), jnp.zeros(tile, jnp.float32)), True
        )
        _, bond, total = lax.fori_loop(
            begin + 1, blocks, lambda block, s: one_block(block, s, False), state
        )
        annuities[date] = ACCRUAL * total
        finals[date] = bond
        return (pos + blocks - begin, numer)

    pos = jnp.int32(0)
    ends = []
    for shard in range(shards):
        skip = lowest[shard]

        def fill(row, pos, shard=shard, skip=skip):
            if shard == 0:
                start = jnp.full(tile, ACCRUAL * curve_ref[row], jnp.float32)
            else:
                start = ACCRUAL * inbox[shard - 1, row_rates + row - low_row]
            rate[shard, row] = start
            res_disc[(pos - skip) * BLOCK + row] = 1.0 / (1.0 + start)
            return pos

        lax.fori_loop(skip * BLOCK, forwards, fill, pos, unroll=BLOCK)
        pos = pos + blocks - skip
        if shard == 0:
            numer = jnp.ones(tile, jnp.float32)
        else:
            numer = inbox[shard - 1, row_numer]
        pos, numer = lax.fori_loop(
            0, per_shard, functools.partial(forward_date, shard), (pos, numer)
        )
        ends.append(numer)

    value = jnp.zeros(tile, jnp.float32)
    for shard in range(shards):
        if shard == 0:
            survive = jnp.ones(tile, jnp.float32)
        else:
            survive = inbox[shard - 1, row_survive]

        def stage(offset, carry, shard=shard):
            survive, value = carry
            date = shard * per_shard + offset
            annuity = annuities[date]
            floating = 1.0 - finals[date]
            slot = slot_ref[date] * basis
            w = [regress_ref[slot + q] for q in range(basis)]
            inverse = 1.0 / annuity
            swap = floating * inverse
            money = (swap - STRIKE) * (1.0 / SMOOTHING)
            exercise = floating - STRIKE * annuity
            inner = w[3] + money * (w[4] + money * w[5])
            continuation = w[0] + money * (w[1] + money * w[2]) + annuity * inner
            sigmoid = jax.nn.sigmoid((exercise - continuation) * (1.0 / SMOOTHING))
            flag = inbox[shard, row_flag + offset]
            chance = flag * sigmoid
            pay = NOTIONAL * exercise / numers[date]
            slope = chance * (1.0 - sigmoid) * (1.0 / SMOOTHING)
            money_adj = (
                w[1] + 2.0 * (w[2] * money) + annuity * (w[4] + 2.0 * (w[5] * money))
            ) * (1.0 / SMOOTHING)
            tilt_money = money_adj * inverse
            seeds_a[2 * date] = slope * (-STRIKE - inner + tilt_money * swap)
            seeds_a[2 * date + 1] = slope * (1.0 - tilt_money)
            chances[date] = chance
            pays[date] = pay
            survs[date] = survive
            value = value + survive * chance * pay
            return (survive * (1.0 - chance), value)

        survive, value = lax.fori_loop(0, per_shard, stage, (survive, value), unroll=5)
    value_ref[...] = value

    gain_adj = jnp.zeros(tile, jnp.float32)
    log_adj = jnp.zeros(tile, jnp.float32)
    for shard in reversed(range(shards)):

        def unwind(step, carry, shard=shard):
            late, log_adj = carry
            date = shard * per_shard + per_shard - 1 - step
            chance = chances[date]
            pay = pays[date]
            survive = survs[date]
            chance_adj = survive * (pay - late)
            direct = (NOTIONAL * survive) * chance / numers[date]
            annuity_adj = chance_adj * seeds_a[2 * date] - STRIKE * direct
            float_adj = chance_adj * seeds_a[2 * date + 1] + direct
            seeds_b[2 * date] = annuity_adj * annuities[date] - float_adj * finals[date]
            seeds_b[2 * date + 1] = ACCRUAL * annuity_adj
            gain = chance * pay
            log_adj = log_adj - survive * gain
            numer_adj[date] = log_adj
            return (gain + late * (1.0 - chance), log_adj)

        gain_adj, log_adj = lax.fori_loop(0, per_shard, unwind, (gain_adj, log_adj), unroll=5)
        if shard > 0:
            log_adj = log_adj * ends[shard - 1] / inbox[shard - 1, row_numer]

    def clear(row, _):
        adjoint[row] = jnp.zeros(tile, jnp.float32)
        return 0

    lax.fori_loop(0, forwards, clear, 0, unroll=BLOCK)

    def backward_date(shard, step, pos):
        date = shard * per_shard + per_shard - 1 - step
        opening = 2 * date + 1
        horizon = horizon_of(date)
        seed_level = seeds_b[2 * date]
        seed_slope = seeds_b[2 * date + 1]
        begin = opening // BLOCK
        here = pos - blocks
        before = here - (blocks - begin)

        def one_block(back, sums):
            sums = list(sums)
            block = blocks - 1 - back
            laters = [adjoint[block * BLOCK + inner] for inner in range(BLOCK)]
            kept = []
            for inner in reversed(range(BLOCK)):
                row = block * BLOCK + inner
                at = (here + block) * BLOCK + inner
                lead = vol_ref[date * forwards + row] * ratio_ref[row]
                old = res_disc[(before + block) * BLOCK + inner]
                pull = (seed_level - seed_slope * res_sum[at]) * (1.0 - res_disc[at])
                inward = laters[inner] - pull
                timed = (horizon * lead) * inward
                sums[0] = sums[0] + timed
                drive_adj = sums[0]
                for f in range(1, factors):
                    scale = scale_ref[(f - 1) * forwards + row]
                    sums[f] = sums[f] + scale * timed
                    drive_adj = drive_adj + scale * sums[f]
                drive_adj = lead * drive_adj
                part = drive_adj * old
                kept.append(
                    (row, inward + (part - part * old), timed * res_tilt[at] + (drive_adj - part))
                )
            for row, earlier, grad in kept:
                adjoint[row] = earlier
                grads[pl.ds((date * forwards + row) * sub, sub)] = grad
            return tuple(sums)

        zero = jnp.zeros(tile, jnp.float32)
        lax.fori_loop(0, blocks - begin, one_block, (zero,) * factors)
        near = jnp.maximum(opening - 2, 0)
        last = opening - 1
        level = numer_adj[date]
        adjoint[near] = level * fixes[2 * date]
        adjoint[last] = level * fixes[2 * date + 1]
        return pos - (blocks - begin)

    for shard in reversed(range(shards)):
        pos = lax.fori_loop(0, per_shard, functools.partial(backward_date, shard), pos)
        pos = pos - (blocks - lowest[shard])
        if shard > 0:

            def cross(row, _, shard=shard):
                start = ACCRUAL * inbox[shard - 1, row_rates + row - low_row]
                adjoint[row] = adjoint[row] * rate[shard - 1, row] / start
                return 0

            lax.fori_loop(2 * shard * per_shard - 1, forwards, cross, 0)

    ones = jnp.ones((8, LANES), jnp.bfloat16)
    width = forwards * sub

    def along(picked):
        return lax.dot_general(
            ones, picked, (((1,), (1,)), ((), ())), preferred_element_type=jnp.float32
        )

    def collect(date, _):
        picked = grads[pl.ds(date * width, forwards, stride=sub)]
        for q in range(1, sub):
            picked = picked + grads[pl.ds(date * width + q, forwards, stride=sub)]
        top = picked.astype(jnp.bfloat16)
        rest = (picked - top.astype(jnp.float32)).astype(jnp.bfloat16)
        vega_ref[pl.ds(date, 1)] = (along(top) + along(rest))[0:1]
        return 0

    lax.fori_loop(0, dates, collect, 0, unroll=4)


def turned(parts, start):
    doubled = jnp.concatenate(parts + parts, axis=0)
    return lax.dynamic_slice_in_dim(doubled, start * parts[0].shape[0], len(parts) * parts[0].shape[0], 0)


def by_source(own, received, place):
    count = len(received) + 1
    return turned([own] + received[::-1], lax.rem(count - place, count))


def exchange(blocks, axis, place):
    count = lax.axis_size(axis)
    own = lax.dynamic_index_in_dim(blocks, place, 0, keepdims=False)
    received = []
    for step in range(1, count):
        sent = lax.dynamic_index_in_dim(blocks, lax.rem(place + step, count), 0, keepdims=False)
        received.append(
            lax.ppermute(sent, axis, [(s, (s + step) % count) for s in range(count)])
        )
    return own, received


def total_over(value, axis):
    count = lax.axis_size(axis)
    if count & (count - 1):
        return lax.psum(value, axis)
    step = 1
    while step < count:
        value = value + lax.ppermute(value, axis, [(s, s ^ step) for s in range(count)])
        step *= 2
    return value


def local(
    start_curve,
    loadings,
    vols,
    shocks,
    exercise_bits,
    regress,
    date_slot,
    ck_rates,
    ck_numer,
    ck_survive,
):
    shards = lax.axis_size("tm")
    groups = lax.axis_size("paths")
    place = lax.axis_index("tm")
    per_shard, forwards = vols.shape
    factors, paths = shocks.shape[1:]
    basis = regress.shape[1]
    dates = shards * per_shard
    per_device = paths // shards
    sub = per_device // LANES
    unit = sub * LANES
    low_row = max(0, (2 * per_shard - 1) // BLOCK * BLOCK)

    def blocked(rows):
        return rows.reshape(-1, shards, sub, LANES).transpose(1, 0, 2, 3)

    small = jnp.concatenate(
        [vols.reshape(-1), regress.reshape(-1), date_slot.astype(jnp.float32)]
    )
    small_rows = -(-small.shape[0] // unit)
    small = jnp.pad(small, (0, small_rows * unit - small.shape[0]))
    payload = jnp.concatenate(
        [
            blocked(shocks.reshape(per_shard * factors, paths)),
            blocked(exercise_bits.astype(jnp.float32)),
            blocked(ck_rates[0, low_row:]),
            blocked(ck_numer),
            blocked(ck_survive),
            jnp.broadcast_to(small.reshape(1, small_rows, sub, LANES), (shards, small_rows, sub, LANES)),
        ],
        axis=1,
    )
    rows = payload.shape[1]
    own, received = exchange(payload, "tm", place)
    smalls = by_source(
        own[rows - small_rows :].reshape(1, -1),
        [part[rows - small_rows :].reshape(1, -1) for part in received],
        place,
    )
    cut = per_shard * forwards
    vol_all = smalls[:, :cut].reshape(-1)
    regress_all = smalls[:, cut : cut + per_shard * basis].reshape(-1)
    slot_all = (
        smalls[:, cut + per_shard * basis : cut + per_shard * (basis + 1)]
        .reshape(-1)
        .astype(jnp.int32)
    )
    loads = loadings / jnp.sqrt(jnp.sum(loadings * loadings, axis=0, keepdims=True))
    ratios = jnp.concatenate([loads[0], 0.5 / loads[0]])
    scales = jnp.broadcast_to(
        (loads[1:] / loads[:1]).reshape(-1, 1, 1), ((factors - 1) * forwards, sub, LANES)
    )

    blocks = forwards // BLOCK
    triangle = sum(blocks - (2 * d + 1) // BLOCK for d in range(dates))
    starts = sum(blocks - max(0, 2 * s * per_shard - 1) // BLOCK for s in range(shards))
    tile = (sub, LANES)
    f32 = jnp.float32
    residual = pltpu.VMEM(((triangle + starts) * BLOCK,) + tile, f32)
    per_date = pltpu.VMEM((dates,) + tile, f32)
    two_per_date = pltpu.VMEM((2 * dates,) + tile, f32)
    per_forward = pltpu.VMEM((forwards,) + tile, f32)
    smem = pl.BlockSpec(memory_space=pltpu.SMEM)
    vega_part, value_part = pl.pallas_call(
        functools.partial(
            kernel,
            shards=shards,
            per_shard=per_shard,
            forwards=forwards,
            factors=factors,
            basis=basis,
            low_row=low_row,
        ),
        out_shape=(
            jax.ShapeDtypeStruct((dates, forwards), f32),
            jax.ShapeDtypeStruct(tile, f32),
        ),
        in_specs=[smem] * 6
        + [pl.BlockSpec(memory_space=pltpu.VMEM)]
        + [pl.BlockSpec(memory_space=pl.ANY)] * shards,
        out_specs=(
            pl.BlockSpec(memory_space=pltpu.VMEM),
            pl.BlockSpec(memory_space=pltpu.VMEM),
        ),
        scratch_shapes=[
            pltpu.VMEM((shards, rows) + tile, f32),
            pltpu.VMEM((shards, forwards) + tile, f32),
            residual,
            residual,
            residual,
            pltpu.VMEM((dates * forwards * sub, LANES), f32),
            per_date,
            per_date,
            per_date,
            two_per_date,
            two_per_date,
            two_per_date,
            per_date,
            per_date,
            per_date,
            per_date,
            per_forward,
            pltpu.SemaphoreType.DMA((shards,)),
        ],
        compiler_params=pltpu.CompilerParams(vmem_limit_bytes=56 * 1024 * 1024),
        name="sweep",
    )(
        place.reshape(1).astype(jnp.int32),
        vol_all,
        ratios,
        regress_all,
        slot_all,
        start_curve,
        scales,
        own,
        *received,
    )

    parts = vega_part.reshape(shards, cut)
    tail = value_part.reshape(1, per_device)
    message = jnp.concatenate([parts, jnp.broadcast_to(tail, (shards, per_device))], axis=1)
    mine, others = exchange(message, "tm", place)
    path_value = by_source(
        mine[cut:].reshape(1, -1), [part[cut:].reshape(1, -1) for part in others], place
    ).reshape(-1)
    summed = mine[:cut]
    for part in others:
        summed = summed + part[:cut]
    summed = total_over(summed.reshape(per_shard, forwards), "paths")
    date = place * per_shard + jnp.arange(per_shard, dtype=jnp.int32)
    alive = jnp.arange(forwards, dtype=jnp.int32)[None, :] >= 2 * date[:, None] + 1
    weight = NOTIONAL / (paths * groups)
    vega = jnp.where(alive, summed * (weight / vols), 0.0)
    return (vega, path_value)


def solution(mesh):
    return jax.shard_map(
        local,
        mesh=mesh,
        in_specs=(
            P(),
            P(),
            P("tm", None),
            P("tm", None, "paths"),
            P("tm", "paths"),
            P("tm", None),
            P("tm"),
            P("tm", None, "paths"),
            P("tm", "paths"),
            P("tm", "paths"),
        ),
        out_specs=(P("tm", None), P("paths")),
        check_vma=False,
    )
```

```python
import functools

import jax
import jax.numpy as jnp
from jax import lax
from jax.experimental import pallas as pl
from jax.experimental.pallas import tpu as pltpu
from jax.sharding import PartitionSpec as P

ACCRUAL = 0.25
STRIKE = 0.04
SMOOTHING = 0.01
NOTIONAL = 100.0
LANES = 128
BLOCK = 8
LOG2E = 1.4426950408889634


class Layout:
    def __init__(self, shards, per_shard, forwards, factors, basis, paths):
        self.shards = shards
        self.per_shard = per_shard
        self.forwards = forwards
        self.factors = factors
        self.basis = basis
        self.per_device = paths // shards
        self.sub = self.per_device // LANES
        self.pairs = -(-per_shard // 2)
        self.low_row = max(0, 2 * per_shard - 1)
        self.shock = 0
        self.flag = self.shock + 2 * self.pairs * factors
        self.rates = self.flag + 2 * self.pairs
        self.numer = self.rates + forwards - self.low_row
        self.survive = self.numer + 1
        small = self.survive + 1
        while (small * self.sub) % 8:
            small += 1
        self.small = small * self.sub
        self.regress_at = per_shard
        self.slot_at = per_shard + basis
        self.small_rows = per_shard + basis + 1
        total = -(-(self.small + self.small_rows) // 8) * 8
        self.flat = total
        self.blocks = forwards // BLOCK


def pack_kernel(place_ref, *refs, lay, count):
    sources = refs[:count]
    out_refs = refs[count : count + lay.shards]
    held = refs[count + lay.shards : 2 * count + lay.shards]
    arrived = refs[-1]
    copies = [
        pltpu.make_async_copy(source, target, arrived.at[index])
        for index, (source, target) in enumerate(zip(sources, held))
    ]
    for copy in copies:
        copy.start()
    for copy in copies:
        copy.wait()
    shock_ref, flag_ref, rate_ref, numer_ref, survive_ref, vol_ref, regress_ref, slot_ref = held
    place = place_ref[0]
    sub = lay.sub
    for step, out in enumerate(out_refs):
        target = lax.rem(place + step, lay.shards)
        for q in range(sub):
            lanes = pl.ds(pl.multiple_of(target * lay.per_device + q * LANES, LANES), LANES)
            for d in range(lay.per_shard):
                row = lay.shock + (d // 2) * lay.factors * 2 + d % 2
                out[pl.ds(row * sub + q, lay.factors, stride=2 * sub), :] = shock_ref[d, :, lanes]
            out[pl.ds(lay.flag * sub + q, lay.per_shard, stride=sub), :] = flag_ref[
                :, lanes
            ].astype(jnp.float32)
            out[
                pl.ds(lay.rates * sub + q, lay.forwards - lay.low_row, stride=sub), :
            ] = rate_ref[0, lay.low_row :, lanes]
            out[pl.ds(lay.numer * sub + q, 1), :] = numer_ref[:, lanes]
            out[pl.ds(lay.survive * sub + q, 1), :] = survive_ref[:, lanes]
        base = lay.small
        out[pl.ds(base, lay.per_shard), :] = jnp.zeros((lay.per_shard, LANES), jnp.float32)
        out[pl.ds(base, lay.per_shard), 0 : lay.forwards] = vol_ref[...]
        out[pl.ds(base + lay.regress_at, lay.basis), 0 : lay.per_shard] = regress_ref[...]
        out[pl.ds(base + lay.slot_at, 1), 0 : lay.per_shard] = slot_ref[...].astype(jnp.float32)


def sweep_kernel(place_ref, curve_ref, table_ref, *refs, lay):
    shards, per_shard, forwards = lay.shards, lay.per_shard, lay.forwards
    factors, basis, sub, blocks, pairs = lay.factors, lay.basis, lay.sub, lay.blocks, lay.pairs
    block_refs = refs[:shards]
    vega_ref, value_ref = refs[shards : shards + 2]
    (
        inbox,
        smalls,
        rate,
        disc,
        res_old,
        res_disc,
        res_tilt,
        res_sum,
        grads,
        annuities,
        finals,
        numers,
        near_fix,
        last_fix,
        float_seed,
        annuity_seed,
        level_seed,
        slope_seed,
        numer_adj,
        survs,
        chances,
        pays,
        adjoint,
        arrived,
        small_arrived,
    ) = refs[shards + 2 :]
    f32 = jnp.float32
    tile = (sub, LANES)
    pair_tile = (2 * sub, LANES)
    place = place_ref[0]
    odd = per_shard % 2
    span = blocks + 2
    state_rows = BLOCK * span * sub
    lowest = [max(0, 2 * s * per_shard - 1) for s in range(shards)]
    is_low = lax.broadcasted_iota(jnp.int32, pair_tile, 0) < sub

    def fetch(step):
        source = lax.rem(place - step + shards, shards)
        return pltpu.make_async_copy(block_refs[step], inbox.at[source], arrived.at[step])

    def fetch_small(step, row):
        source = lax.rem(place - step + shards, shards)
        spot = (source * lay.small_rows + row) * LANES
        return pltpu.make_async_copy(
            block_refs[step].at[lay.small + row],
            smalls.at[pl.ds(pl.multiple_of(spot, LANES), LANES)],
            small_arrived.at[step, row],
        )

    for step in range(shards):
        fetch(step).start()
        for row in range(lay.small_rows):
            fetch_small(step, row).start()

    def clear(ref):
        rows = ref.shape[0]

        def one(row, _):
            ref[pl.ds(pl.multiple_of(row * 8, 8), 8)] = jnp.zeros((8, LANES), f32)
            return 0

        lax.fori_loop(0, rows // 8, one, 0, unroll=8)

    clear(rate)
    clear(disc)
    clear(adjoint)

    for step in range(shards):
        fetch(step).wait()
        for row in range(lay.small_rows):
            fetch_small(step, row).wait()

    def mail(shard, row, count=1):
        return inbox[shard, pl.ds(row * sub, count * sub)]

    def place_of(row):
        if isinstance(row, int):
            return (row % BLOCK * span + blocks - row // BLOCK) * sub
        return (lax.rem(row, BLOCK) * span + blocks - lax.div(row, BLOCK)) * sub

    def state(ref, row, shard=0):
        return ref[pl.ds(shard * state_rows + place_of(row), sub)]

    def slot_of(shard, offset):
        return (shard * 2 * pairs + offset) * sub

    def both(low, high):
        return jnp.where(is_low, low, high)

    def horizons(date):
        return both(jnp.where(date == 0, ACCRUAL, 2.0 * ACCRUAL), 2.0 * ACCRUAL)

    def opening_pair(shard, offset):
        opening = 2 * (shard * per_shard + offset) + 1
        second = opening + 2
        if odd:
            second = jnp.where(offset + 1 < per_shard, second, 4 * forwards)
        return opening, second

    inner_of = [
        both(0, BLOCK) - inner for inner in range(BLOCK)
    ]

    def volatility(shard, offset, block, limit):
        base = (shard * lay.small_rows + offset) * LANES + block * BLOCK
        first = jnp.broadcast_to(block * BLOCK, pair_tile)
        found = []
        for inner in range(BLOCK):
            raw = both(smalls[base + inner], smalls[base + (LANES - BLOCK + inner)])
            found.append(jnp.where(first >= limit + inner_of[inner], raw, 0.0))
        return found

    def table(kind, row):
        return table_ref[kind * (forwards + BLOCK) + row]

    def forward_pair(shard, index, carry):
        pos, numer = carry
        offset = 2 * index
        date = shard * per_shard + offset
        opening, second = opening_pair(shard, offset)
        limit = both(opening, second)
        begin = opening // BLOCK
        horizon = horizons(date)
        timer = horizon * LOG2E
        root = both(jnp.where(date == 0, ACCRUAL**-0.5, (2.0 * ACCRUAL) ** -0.5), (2.0 * ACCRUAL) ** -0.5)
        sums = tuple(
            mail(shard, lay.shock + (index * factors + f) * 2, 2) * root for f in range(factors)
        )

        if odd:
            real = is_low | (offset + 1 < per_shard)
            sums = tuple(jnp.where(real, part, 0.0) for part in sums)

        def one_block(step, held):
            sums, bond, total = held
            sums = list(sums)
            block = begin + step
            at = (pos + step) * BLOCK
            spots = [(inner * span + blocks - block) * sub for inner in range(BLOCK)]
            sigmas = volatility(shard, offset, block, limit)
            rates = [rate[pl.ds(shard * state_rows + spot, 2 * sub)] for spot in spots]
            olds = [disc[pl.ds(spot, 2 * sub)] for spot in spots]
            kept = []
            for inner in range(BLOCK):
                row = block * BLOCK + inner
                sigma = sigmas[inner]
                lead = sigma * table(0, row)
                half = sigma * table(1, row)
                drive = lead - lead * olds[inner]
                sums[0] = sums[0] + drive
                tilt = sums[0]
                for f in range(1, factors):
                    scale = table(1 + f, row)
                    sums[f] = sums[f] + scale * drive
                    tilt = tilt + scale * sums[f]
                tilt = tilt - half
                new = rates[inner] * jnp.exp2((timer * lead) * tilt)
                fresh = 1.0 / (1.0 + new)
                alive = sigma > 0.0
                shown = jnp.where(alive, fresh, 1.0)
                kept.append((new, fresh, shown, tilt - half, total))
                bond = bond * shown
                total = total + jnp.where(alive, bond, 0.0)
            for inner, (new, fresh, shown, lean, before) in enumerate(kept):
                rate[pl.ds(shard * state_rows + spots[inner], 2 * sub)] = new
                disc[pl.ds(spots[inner], 2 * sub)] = fresh
                res_old[at + inner] = olds[inner]
                res_disc[at + inner] = shown
                res_tilt[at + inner] = lean
                res_sum[at + inner] = before
            return (tuple(sums), bond, total)

        steps = blocks - begin + 1
        _, bond, total = lax.fori_loop(
            0, steps, one_block, (sums, jnp.ones(pair_tile, f32), jnp.zeros(pair_tile, f32))
        )
        slot = slot_of(shard, offset)
        annuities[pl.ds(slot, 2 * sub)] = ACCRUAL * total
        finals[pl.ds(slot, 2 * sub)] = bond
        near = jnp.maximum(opening - 2, 0)
        numer = numer * (1.0 + state(rate, opening - 1, shard))
        numer = numer * jnp.where(date == 0, 1.0, 1.0 + state(rate, near, shard))
        numers[pl.ds(slot, sub)] = numer
        later = numer * (1.0 + state(rate, opening, shard)) * (
            1.0 + state(rate, opening + 1, shard)
        )
        if odd:
            later = jnp.where(offset + 1 < per_shard, later, numer)
        numers[pl.ds(slot + sub, sub)] = later
        near_fix[pl.ds(slot, sub)] = 1.0 - state(disc, near)
        last_fix[pl.ds(slot, sub)] = 1.0 - state(disc, opening - 1)
        near_fix[pl.ds(slot + sub, sub)] = 1.0 - state(disc, opening)
        last_fix[pl.ds(slot + sub, sub)] = 1.0 - state(disc, opening + 1)
        return (pos + steps, later)

    pos = jnp.int32(0)
    ends = []
    for shard in range(shards):

        for row in range(lowest[shard], forwards):
            if shard == 0:
                start = jnp.full(tile, ACCRUAL * curve_ref[row], f32)
            else:
                start = ACCRUAL * mail(shard - 1, lay.rates + row - lay.low_row)
            rate[pl.ds(shard * state_rows + place_of(row), sub)] = start
            disc[pl.ds(place_of(row), sub)] = 1.0 / (1.0 + start)
        numer = jnp.ones(tile, f32) if shard == 0 else mail(shard - 1, lay.numer)
        pos, numer = lax.fori_loop(
            0, pairs, functools.partial(forward_pair, shard), (pos, numer)
        )
        ends.append(numer)

    value = jnp.zeros(tile, f32)
    for shard in range(shards):

        def stage(index, _, shard=shard):
            offset = 2 * index
            slot = slot_of(shard, offset)
            pair = pl.ds(slot, 2 * sub)
            annuity = annuities[pair]
            floating = 1.0 - finals[pair]
            marks = []
            for step in range(2):
                spot = jnp.minimum(offset + step, per_shard - 1)
                named = smalls[(shard * lay.small_rows + lay.slot_at) * LANES + spot]
                named = named.astype(jnp.int32)
                owner = lax.div(named, per_shard)
                base = (owner * lay.small_rows + lay.regress_at) * LANES
                base = base + lax.rem(named, per_shard)
                marks.append([smalls[base + q * LANES] for q in range(basis)])
            w = [both(marks[0][q], marks[1][q]) for q in range(basis)]
            if odd:
                real = is_low | (offset + 1 < per_shard)
                annuity = jnp.where(real, annuity, 1.0)
            inverse = 1.0 / annuity
            swap = floating * inverse
            money = (swap - STRIKE) * (1.0 / SMOOTHING)
            exercise = floating - STRIKE * annuity
            inner = w[3] + money * (w[4] + money * w[5])
            continuation = w[0] + money * (w[1] + money * w[2]) + annuity * inner
            sigmoid = jax.nn.sigmoid((exercise - continuation) * (1.0 / SMOOTHING))
            flag = mail(shard, lay.flag + offset, 2)
            if odd:
                flag = jnp.where(real, flag, 0.0)
            chance = flag * sigmoid
            slope = chance * (1.0 - sigmoid) * (1.0 / SMOOTHING)
            money_adj = (
                w[1] + 2.0 * (w[2] * money) + annuity * (w[4] + 2.0 * (w[5] * money))
            ) * (1.0 / SMOOTHING)
            tilt_money = money_adj * inverse
            annuity_seed[pair] = slope * (-STRIKE - inner + tilt_money * swap)
            float_seed[pair] = slope * (1.0 - tilt_money)
            chances[pair] = chance
            pays[pair] = NOTIONAL * exercise / numers[pair]
            return 0

        lax.fori_loop(0, pairs, stage, 0, unroll=pairs)
        survive = jnp.ones(tile, f32) if shard == 0 else mail(shard - 1, lay.survive)

        def gain(offset, carry, shard=shard):
            survive, value = carry
            here = pl.ds(slot_of(shard, offset), sub)
            chance = chances[here]
            survs[here] = survive
            return (survive * (1.0 - chance), value + survive * chance * pays[here])

        survive, value = lax.fori_loop(0, per_shard, gain, (survive, value), unroll=per_shard)
    value_ref[...] = value

    late = jnp.zeros(tile, f32)
    log_adj = jnp.zeros(tile, f32)
    for shard in reversed(range(shards)):

        def unwind(step, carry, shard=shard):
            late, log_adj = carry
            here = pl.ds(slot_of(shard, per_shard - 1 - step), sub)
            chance = chances[here]
            pay = pays[here]
            survive = survs[here]
            chance_adj = survive * (pay - late)
            direct = (NOTIONAL * survive) * chance / numers[here]
            annuity_adj = chance_adj * annuity_seed[here] - STRIKE * direct
            float_adj = chance_adj * float_seed[here] + direct
            level_seed[here] = annuity_adj * annuities[here] - float_adj * finals[here]
            slope_seed[here] = ACCRUAL * annuity_adj
            gained = chance * pay
            log_adj = log_adj - survive * gained
            numer_adj[here] = log_adj
            return (gained + late * (1.0 - chance), log_adj)

        late, log_adj = lax.fori_loop(0, per_shard, unwind, (late, log_adj), unroll=per_shard)
        if odd:
            here = pl.ds(slot_of(shard, per_shard), sub)
            level_seed[here] = jnp.zeros(tile, f32)
            slope_seed[here] = jnp.zeros(tile, f32)
        if shard > 0:
            log_adj = log_adj * ends[shard - 1] / mail(shard - 1, lay.numer)

    def backward_pair(shard, back, pos):
        index = pairs - 1 - back
        offset = 2 * index
        date = shard * per_shard + offset
        opening, second = opening_pair(shard, offset)
        limit = both(opening, second)
        begin = opening // BLOCK
        horizon = horizons(date)
        slot = slot_of(shard, offset)
        level = level_seed[pl.ds(slot, 2 * sub)]
        slope = slope_seed[pl.ds(slot, 2 * sub)]
        steps = blocks - begin + 1
        first = pos - steps
        bank = (shard * pairs + index) * (blocks + 1)

        def one_block(turn, sums):
            sums = list(sums)
            step = steps - 1 - turn
            block = begin + step
            at = (first + step) * BLOCK
            spots = [(inner * span + blocks - block) * sub for inner in range(BLOCK)]
            sigmas = volatility(shard, offset, block, limit)
            laters = [adjoint[pl.ds(spot, 2 * sub)] for spot in spots]
            kept = []
            for inner in reversed(range(BLOCK)):
                row = block * BLOCK + inner
                lead = sigmas[inner] * table(0, row)
                old = res_old[at + inner]
                pull = (level - slope * res_sum[at + inner]) * (1.0 - res_disc[at + inner])
                inward = laters[inner] - pull
                timed = (horizon * lead) * inward
                sums[0] = sums[0] + timed
                drive_adj = sums[0]
                for f in range(1, factors):
                    scale = table(1 + f, row)
                    sums[f] = sums[f] + scale * timed
                    drive_adj = drive_adj + scale * sums[f]
                drive_adj = lead * drive_adj
                part = drive_adj * old
                kept.append(
                    (
                        inner,
                        inward + (part - part * old),
                        timed * res_tilt[at + inner] + (drive_adj - part),
                    )
                )
            for inner, earlier, grad in kept:
                adjoint[pl.ds(spots[inner], 2 * sub)] = earlier
                grads[
                    pl.ds(pl.multiple_of(((bank + block) * BLOCK + inner) * 2 * sub, 2 * sub), 2 * sub)
                ] = grad
            return tuple(sums)

        def patch(row, slot, fix):
            adjoint[pl.ds(place_of(row), sub)] = numer_adj[pl.ds(slot, sub)] * fix[pl.ds(slot, sub)]

        sums = (jnp.zeros(pair_tile, f32),) * factors
        turn = steps - 1 - ((opening + 1) // BLOCK - begin)
        sums = lax.fori_loop(0, turn, one_block, sums)

        def patch_second():
            patch(opening, slot + sub, near_fix)
            patch(opening + 1, slot + sub, last_fix)

        if odd:
            pl.when(offset + 1 < per_shard)(patch_second)
        else:
            patch_second()
        lax.fori_loop(turn, steps, one_block, sums)
        patch(jnp.maximum(opening - 2, 0), slot, near_fix)
        patch(opening - 1, slot, last_fix)
        return first

    for shard in reversed(range(shards)):
        pos = lax.fori_loop(0, pairs, functools.partial(backward_pair, shard), pos)
        if shard > 0:

            for row in range(lowest[shard], forwards):
                start = ACCRUAL * mail(shard - 1, lay.rates + row - lay.low_row)
                here = pl.ds(place_of(row), sub)
                adjoint[here] = adjoint[here] * state(rate, row, shard - 1) / start

    ones = jnp.ones((LANES, LANES), jnp.bfloat16)
    rows = forwards + BLOCK
    on_diagonal = lax.broadcasted_iota(jnp.int32, (rows, LANES), 0) == lax.broadcasted_iota(
        jnp.int32, (rows, LANES), 1
    )

    def along(picked):
        return jnp.dot(picked, ones, preferred_element_type=f32)

    def collect(pair, _):
        base = pair * (rows * 2 * sub)
        for half in range(2):
            picked = grads[pl.ds(base + half * sub, rows, stride=2 * sub)]
            for q in range(1, sub):
                picked = picked + grads[pl.ds(base + half * sub + q, rows, stride=2 * sub)]
            top = picked.astype(jnp.bfloat16)
            rest = (picked - top.astype(f32)).astype(jnp.bfloat16)
            total = jnp.where(on_diagonal, along(top) + along(rest), 0.0)
            line = jnp.sum(total, axis=0, keepdims=True)
            vega_ref[pl.ds(2 * pair + half, 1)] = line[:, half * BLOCK : half * BLOCK + forwards]
        return 0

    lax.fori_loop(0, shards * pairs, collect, 0, unroll=2)


def by_source(own, received, place):
    count = len(received) + 1
    parts = [own] + received[::-1]
    doubled = jnp.concatenate(parts + parts, axis=0)
    start = lax.rem(count - place, count) * own.shape[0]
    return lax.dynamic_slice_in_dim(doubled, start, count * own.shape[0], 0)


def shifted(value, axis, step):
    count = lax.axis_size(axis)
    return lax.ppermute(value, axis, [(s, (s + step) % count) for s in range(count)])


def total_over(value, axis):
    count = lax.axis_size(axis)
    if count & (count - 1):
        return lax.psum(value, axis)
    step = 1
    while step < count:
        masks = [step]
        if step > 1 and 2 * step < count:
            masks = [step, 2 * step, 3 * step]
        heard = [lax.ppermute(value, axis, [(s, s ^ mask) for s in range(count)]) for mask in masks]
        value = value + heard[0]
        if len(heard) > 1:
            value = value + (heard[1] + heard[2])
        step *= 2 if len(masks) == 1 else 4
    return value


def local(
    start_curve,
    loadings,
    vols,
    shocks,
    exercise_bits,
    regress,
    date_slot,
    ck_rates,
    ck_numer,
    ck_survive,
):
    shards = lax.axis_size("tm")
    groups = lax.axis_size("paths")
    place = lax.axis_index("tm")
    per_shard, forwards = vols.shape
    factors, paths = shocks.shape[1:]
    lay = Layout(shards, per_shard, forwards, factors, regress.shape[1], paths)
    sub, blocks, pairs = lay.sub, lay.blocks, lay.pairs
    f32 = jnp.float32
    smem = pl.BlockSpec(memory_space=pltpu.SMEM)
    vmem = pl.BlockSpec(memory_space=pltpu.VMEM)
    spot = place.reshape(1).astype(jnp.int32)

    sources = (
        shocks,
        exercise_bits,
        ck_rates,
        ck_numer,
        ck_survive,
        vols,
        regress.T,
        date_slot.reshape(1, per_shard),
    )
    sources = tuple(pltpu.with_memory_space_constraint(source, pltpu.HBM) for source in sources)
    messages = pl.pallas_call(
        functools.partial(pack_kernel, lay=lay, count=len(sources)),
        out_shape=[jax.ShapeDtypeStruct((lay.flat, LANES), f32)] * shards,
        in_specs=[smem] + [pl.BlockSpec(memory_space=pltpu.HBM)] * len(sources),
        out_specs=[vmem] * shards,
        scratch_shapes=[pltpu.VMEM(source.shape, source.dtype) for source in sources]
        + [pltpu.SemaphoreType.DMA((len(sources),))],
        compiler_params=pltpu.CompilerParams(vmem_limit_bytes=16 * 1024 * 1024),
        name="pack",
    )(spot, *sources)
    received = [shifted(messages[step], "tm", step) for step in range(1, shards)]

    loads = loadings / jnp.sqrt(jnp.sum(loadings * loadings, axis=0, keepdims=True))
    kinds = jnp.concatenate([loads[:1], 0.5 / loads[:1], loads[1:] / loads[:1]])
    ahead = jnp.pad(kinds, ((0, 0), (0, BLOCK)), constant_values=1.0)
    behind = jnp.pad(kinds, ((0, 0), (BLOCK, 0)), constant_values=1.0)
    tables = jnp.broadcast_to(
        jnp.stack([ahead, behind], axis=-1).reshape(-1, 2, 1, 1),
        (kinds.shape[0] * (forwards + BLOCK), 2, sub, LANES),
    ).reshape(-1, 2 * sub, LANES)

    iterations = sum(
        blocks - (2 * (s * per_shard + 2 * k) + 1) // BLOCK + 1
        for s in range(shards)
        for k in range(pairs)
    )
    residual = pltpu.VMEM((iterations * BLOCK, 2 * sub, LANES), f32)
    per_slot = pltpu.VMEM((shards * 2 * pairs * sub, LANES), f32)
    state_rows = BLOCK * (blocks + 2) * sub
    vega_part, value_part = pl.pallas_call(
        functools.partial(sweep_kernel, lay=lay),
        out_shape=(
            jax.ShapeDtypeStruct((shards * 2 * pairs, forwards), f32),
            jax.ShapeDtypeStruct((sub, LANES), f32),
        ),
        in_specs=[smem, smem, vmem] + [pl.BlockSpec(memory_space=pl.ANY)] * shards,
        out_specs=(vmem, vmem),
        scratch_shapes=[
            pltpu.VMEM((shards, lay.flat, LANES), f32),
            pltpu.SMEM((shards * lay.small_rows * LANES,), f32),
            pltpu.VMEM((shards * state_rows, LANES), f32),
            pltpu.VMEM((state_rows, LANES), f32),
            residual,
            residual,
            residual,
            residual,
            pltpu.VMEM((shards * pairs * (blocks + 1) * BLOCK * 2 * sub, LANES), f32),
        ]
        + [per_slot] * 13
        + [
            pltpu.VMEM((state_rows, LANES), f32),
            pltpu.SemaphoreType.DMA((shards,)),
            pltpu.SemaphoreType.DMA((shards, lay.small_rows)),
        ],
        compiler_params=pltpu.CompilerParams(vmem_limit_bytes=48 * 1024 * 1024),
        name="sweep",
    )(spot, start_curve, tables, messages[0], *received)

    parts = vega_part.reshape(shards, 2 * pairs, forwards)[:, :per_shard].reshape(shards, -1)
    cut = per_shard * forwards
    tail = jnp.broadcast_to(value_part.reshape(1, -1), (shards, lay.per_device))
    message = jnp.concatenate([parts, tail], axis=1)
    mine = lax.dynamic_index_in_dim(message, place, 0, keepdims=False)
    others = []
    for step in range(1, shards):
        sent = lax.dynamic_index_in_dim(message, lax.rem(place + step, shards), 0, keepdims=False)
        others.append(shifted(sent, "tm", step))
    path_value = by_source(
        mine[cut:].reshape(1, -1), [part[cut:].reshape(1, -1) for part in others], place
    ).reshape(-1)
    summed = mine[:cut]
    for part in others:
        summed = summed + part[:cut]
    summed = total_over(summed.reshape(per_shard, forwards), "paths")
    date = place * per_shard + jnp.arange(per_shard, dtype=jnp.int32)
    alive = jnp.arange(forwards, dtype=jnp.int32)[None, :] >= 2 * date[:, None] + 1
    weight = NOTIONAL / (paths * groups)
    vega = jnp.where(alive, summed * (weight / vols), 0.0)
    return (vega, path_value)


def solution(mesh):
    return jax.shard_map(
        local,
        mesh=mesh,
        in_specs=(
            P(),
            P(),
            P("tm", None),
            P("tm", None, "paths"),
            P("tm", "paths"),
            P("tm", None),
            P("tm"),
            P("tm", None, "paths"),
            P("tm", "paths"),
            P("tm", "paths"),
        ),
        out_specs=(P("tm", None), P("paths")),
        check_vma=False,
    )
```

```python
import functools

import jax
import jax.numpy as jnp
from jax import lax
from jax.experimental import pallas as pl
from jax.experimental.pallas import tpu as pltpu
from jax.sharding import PartitionSpec as P

ACCRUAL = 0.25
STRIKE = 0.04
SMOOTHING = 0.01
NOTIONAL = 100.0
LANES = 128
BLOCK = 8
LOG2E = 1.4426950408889634


class Layout:
    def __init__(self, shards, per_shard, forwards, factors, basis, paths):
        self.shards = shards
        self.per_shard = per_shard
        self.forwards = forwards
        self.factors = factors
        self.basis = basis
        self.per_device = paths // shards
        self.sub = self.per_device // LANES
        self.pairs = -(-per_shard // 2)
        self.low_row = max(0, 2 * per_shard - 1)
        self.shock = 0
        self.flag = self.shock + 2 * self.pairs * factors
        self.rates = self.flag + 2 * self.pairs
        self.numer = self.rates + forwards - self.low_row
        self.survive = self.numer + 1
        small = self.survive + 1
        while (small * self.sub) % 8:
            small += 1
        self.small = small * self.sub
        self.regress_at = per_shard
        self.slot_at = per_shard + basis
        self.small_rows = per_shard + basis + 1
        total = -(-(self.small + self.small_rows) // 8) * 8
        self.flat = total
        self.blocks = forwards // BLOCK


def pack_kernel(place_ref, *refs, lay, count):
    sources = refs[:count]
    out_refs = refs[count : count + lay.shards]
    held = refs[count + lay.shards : 2 * count + lay.shards]
    arrived = refs[-1]
    copies = [
        pltpu.make_async_copy(source, target, arrived.at[index])
        for index, (source, target) in enumerate(zip(sources, held))
    ]
    for copy in copies:
        copy.start()
    for copy in copies:
        copy.wait()
    shock_ref, flag_ref, rate_ref, numer_ref, survive_ref, vol_ref, regress_ref, slot_ref = held
    place = place_ref[0]
    sub = lay.sub
    for step, out in enumerate(out_refs):
        target = lax.rem(place + step, lay.shards)
        for q in range(sub):
            lanes = pl.ds(pl.multiple_of(target * lay.per_device + q * LANES, LANES), LANES)
            for d in range(lay.per_shard):
                row = lay.shock + (d // 2) * lay.factors * 2 + d % 2
                out[pl.ds(row * sub + q, lay.factors, stride=2 * sub), :] = shock_ref[d, :, lanes]
            out[pl.ds(lay.flag * sub + q, lay.per_shard, stride=sub), :] = flag_ref[
                :, lanes
            ].astype(jnp.float32)
            out[
                pl.ds(lay.rates * sub + q, lay.forwards - lay.low_row, stride=sub), :
            ] = rate_ref[0, lay.low_row :, lanes]
            out[pl.ds(lay.numer * sub + q, 1), :] = numer_ref[:, lanes]
            out[pl.ds(lay.survive * sub + q, 1), :] = survive_ref[:, lanes]
        base = lay.small
        out[pl.ds(base, lay.per_shard), :] = jnp.zeros((lay.per_shard, LANES), jnp.float32)
        out[pl.ds(base, lay.per_shard), 0 : lay.forwards] = vol_ref[...]
        out[pl.ds(base + lay.regress_at, lay.basis), 0 : lay.per_shard] = regress_ref[...]
        out[pl.ds(base + lay.slot_at, 1), 0 : lay.per_shard] = slot_ref[...].astype(jnp.float32)


def sweep_kernel(place_ref, curve_ref, table_ref, *refs, lay):
    shards, per_shard, forwards = lay.shards, lay.per_shard, lay.forwards
    factors, basis, sub, blocks, pairs = lay.factors, lay.basis, lay.sub, lay.blocks, lay.pairs
    block_refs = refs[:shards]
    vega_ref, value_ref = refs[shards : shards + 2]
    (
        inbox,
        smalls,
        rate,
        disc,
        res_old,
        res_disc,
        res_tilt,
        res_sum,
        res_lead,
        grads,
        annuities,
        finals,
        numers,
        near_fix,
        last_fix,
        float_seed,
        annuity_seed,
        level_seed,
        slope_seed,
        numer_adj,
        survs,
        chances,
        pays,
        adjoint,
        arrived,
        small_arrived,
    ) = refs[shards + 2 :]
    f32 = jnp.float32
    tile = (sub, LANES)
    pair_tile = (2 * sub, LANES)
    place = place_ref[0]
    odd = per_shard % 2
    span = blocks + 2
    state_rows = BLOCK * span * sub
    lowest = [max(0, 2 * s * per_shard - 1) for s in range(shards)]
    side = lax.broadcasted_iota(jnp.int32, pair_tile, 0)
    is_low = side < sub

    def fetch(step):
        source = lax.rem(place - step + shards, shards)
        return pltpu.make_async_copy(block_refs[step], inbox.at[source], arrived.at[step])

    def fetch_small(step, row):
        source = lax.rem(place - step + shards, shards)
        spot = (source * lay.small_rows + row) * LANES
        return pltpu.make_async_copy(
            block_refs[step].at[lay.small + row],
            smalls.at[pl.ds(pl.multiple_of(spot, LANES), LANES)],
            small_arrived.at[step, row],
        )

    for step in range(shards):
        fetch(step).start()
        for row in range(lay.small_rows):
            fetch_small(step, row).start()

    def clear(ref):
        rows = ref.shape[0]

        def one(row, _):
            ref[pl.ds(pl.multiple_of(row * 8, 8), 8)] = jnp.zeros((8, LANES), f32)
            return 0

        lax.fori_loop(0, rows // 8, one, 0, unroll=8)

    clear(rate)
    clear(disc)
    clear(adjoint)

    for step in range(shards):
        fetch(step).wait()
        for row in range(lay.small_rows):
            fetch_small(step, row).wait()

    def mail(shard, row, count=1):
        return inbox[shard, pl.ds(row * sub, count * sub)]

    def place_of(row):
        if isinstance(row, int):
            return (row % BLOCK * span + blocks - row // BLOCK) * sub
        return (lax.rem(row, BLOCK) * span + blocks - lax.div(row, BLOCK)) * sub

    def state(ref, row, shard=0):
        return ref[pl.ds(shard * state_rows + place_of(row), sub)]

    def slot_of(shard, offset):
        return (shard * 2 * pairs + offset) * sub

    def both(low, high):
        return jnp.where(is_low, low, high)

    def horizons(date):
        return both(jnp.where(date == 0, ACCRUAL, 2.0 * ACCRUAL), 2.0 * ACCRUAL)

    def opening_pair(shard, offset):
        opening = 2 * (shard * per_shard + offset) + 1
        second = opening + 2
        if odd:
            second = jnp.where(offset + 1 < per_shard, second, 4 * forwards)
        return opening, second

    def volatility(shard, offset, block, reach):
        base = (shard * lay.small_rows + offset) * LANES + block * BLOCK
        beyond = block * BLOCK - reach
        found = []
        for inner in range(BLOCK):
            raw = both(smalls[base + inner], smalls[base + (LANES - BLOCK + inner)])
            found.append(jnp.where(beyond >= -inner, raw, 0.0))
        return found

    def table(kind, row):
        return table_ref[kind * (forwards + BLOCK) + row]

    def forward_pair(shard, index, carry):
        pos, numer = carry
        offset = 2 * index
        date = shard * per_shard + offset
        opening, second = opening_pair(shard, offset)
        reach = both(opening, second + BLOCK)
        begin = opening // BLOCK
        horizon = horizons(date)
        timer = horizon * LOG2E
        root = both(jnp.where(date == 0, ACCRUAL**-0.5, (2.0 * ACCRUAL) ** -0.5), (2.0 * ACCRUAL) ** -0.5)
        sums = tuple(
            mail(shard, lay.shock + (index * factors + f) * 2, 2) * root for f in range(factors)
        )

        if odd:
            real = is_low | (offset + 1 < per_shard)
            sums = tuple(jnp.where(real, part, 0.0) for part in sums)

        def one_block(step, held):
            sums, bond, total = held
            sums = list(sums)
            block = begin + step
            at = (pos + step) * BLOCK
            spots = [(blocks - block) * sub + inner * (span * sub) for inner in range(BLOCK)]
            sigmas = volatility(shard, offset, block, reach)
            rates = [rate[pl.ds(shard * state_rows + spot, 2 * sub)] for spot in spots]
            olds = [disc[pl.ds(spot, 2 * sub)] for spot in spots]
            kept = []
            for inner in range(BLOCK):
                row = block * BLOCK + inner
                sigma = sigmas[inner]
                lead = sigma * table(0, row)
                half = sigma * table(1, row)
                drive = lead - lead * olds[inner]
                sums[0] = sums[0] + drive
                tilt = sums[0]
                for f in range(1, factors):
                    scale = table(1 + f, row)
                    sums[f] = sums[f] + scale * drive
                    tilt = tilt + scale * sums[f]
                tilt = tilt - half
                new = rates[inner] * jnp.exp2((timer * lead) * tilt)
                fresh = 1.0 / (1.0 + new)
                alive = sigma > 0.0
                shown = jnp.where(alive, fresh, 1.0)
                kept.append((new, fresh, shown, tilt - half, total, lead))
                bond = bond * shown
                total = total + jnp.where(alive, bond, 0.0)
            for inner, (new, fresh, shown, lean, before, lead) in enumerate(kept):
                rate[pl.ds(shard * state_rows + spots[inner], 2 * sub)] = new
                disc[pl.ds(spots[inner], 2 * sub)] = fresh
                res_old[at + inner] = olds[inner]
                res_disc[at + inner] = shown
                res_tilt[at + inner] = lean
                res_sum[at + inner] = before
                res_lead[at + inner] = lead
            return (tuple(sums), bond, total)

        steps = blocks - begin + 1
        _, bond, total = lax.fori_loop(
            0, steps, one_block, (sums, jnp.ones(pair_tile, f32), jnp.zeros(pair_tile, f32))
        )
        slot = slot_of(shard, offset)
        annuities[pl.ds(slot, 2 * sub)] = ACCRUAL * total
        finals[pl.ds(slot, 2 * sub)] = bond
        near = jnp.maximum(opening - 2, 0)
        numer = numer * (1.0 + state(rate, opening - 1, shard))
        numer = numer * jnp.where(date == 0, 1.0, 1.0 + state(rate, near, shard))
        numers[pl.ds(slot, sub)] = numer
        later = numer * (1.0 + state(rate, opening, shard)) * (
            1.0 + state(rate, opening + 1, shard)
        )
        if odd:
            later = jnp.where(offset + 1 < per_shard, later, numer)
        numers[pl.ds(slot + sub, sub)] = later
        near_fix[pl.ds(slot, sub)] = 1.0 - state(disc, near)
        last_fix[pl.ds(slot, sub)] = 1.0 - state(disc, opening - 1)
        near_fix[pl.ds(slot + sub, sub)] = 1.0 - state(disc, opening)
        last_fix[pl.ds(slot + sub, sub)] = 1.0 - state(disc, opening + 1)
        return (pos + steps, later)

    pos = jnp.int32(0)
    ends = []
    for shard in range(shards):

        for row in range(lowest[shard], forwards):
            if shard == 0:
                start = jnp.full(tile, ACCRUAL * curve_ref[row], f32)
            else:
                start = ACCRUAL * mail(shard - 1, lay.rates + row - lay.low_row)
            rate[pl.ds(shard * state_rows + place_of(row), sub)] = start
            disc[pl.ds(place_of(row), sub)] = 1.0 / (1.0 + start)
        numer = jnp.ones(tile, f32) if shard == 0 else mail(shard - 1, lay.numer)
        pos, numer = lax.fori_loop(
            0, pairs, functools.partial(forward_pair, shard), (pos, numer)
        )
        ends.append(numer)

    value = jnp.zeros(tile, f32)
    for shard in range(shards):

        def stage(index, _, shard=shard):
            offset = 2 * index
            slot = slot_of(shard, offset)
            pair = pl.ds(slot, 2 * sub)
            annuity = annuities[pair]
            floating = 1.0 - finals[pair]
            marks = []
            for step in range(2):
                spot = jnp.minimum(offset + step, per_shard - 1)
                named = smalls[(shard * lay.small_rows + lay.slot_at) * LANES + spot]
                named = named.astype(jnp.int32)
                owner = lax.div(named, per_shard)
                base = (owner * lay.small_rows + lay.regress_at) * LANES
                base = base + lax.rem(named, per_shard)
                marks.append([smalls[base + q * LANES] for q in range(basis)])
            w = [both(marks[0][q], marks[1][q]) for q in range(basis)]
            if odd:
                real = is_low | (offset + 1 < per_shard)
                annuity = jnp.where(real, annuity, 1.0)
            inverse = 1.0 / annuity
            swap = floating * inverse
            money = (swap - STRIKE) * (1.0 / SMOOTHING)
            exercise = floating - STRIKE * annuity
            inner = w[3] + money * (w[4] + money * w[5])
            continuation = w[0] + money * (w[1] + money * w[2]) + annuity * inner
            sigmoid = jax.nn.sigmoid((exercise - continuation) * (1.0 / SMOOTHING))
            flag = mail(shard, lay.flag + offset, 2)
            if odd:
                flag = jnp.where(real, flag, 0.0)
            chance = flag * sigmoid
            slope = chance * (1.0 - sigmoid) * (1.0 / SMOOTHING)
            money_adj = (
                w[1] + 2.0 * (w[2] * money) + annuity * (w[4] + 2.0 * (w[5] * money))
            ) * (1.0 / SMOOTHING)
            tilt_money = money_adj * inverse
            annuity_seed[pair] = slope * (-STRIKE - inner + tilt_money * swap)
            float_seed[pair] = slope * (1.0 - tilt_money)
            chances[pair] = chance
            pays[pair] = NOTIONAL * exercise / numers[pair]
            return 0

        lax.fori_loop(0, pairs, stage, 0, unroll=pairs)
        survive = jnp.ones(tile, f32) if shard == 0 else mail(shard - 1, lay.survive)

        def gain(offset, carry, shard=shard):
            survive, value = carry
            here = pl.ds(slot_of(shard, offset), sub)
            chance = chances[here]
            survs[here] = survive
            return (survive * (1.0 - chance), value + survive * chance * pays[here])

        survive, value = lax.fori_loop(0, per_shard, gain, (survive, value), unroll=per_shard)
    value_ref[...] = value

    late = jnp.zeros(tile, f32)
    log_adj = jnp.zeros(tile, f32)
    for shard in reversed(range(shards)):

        def unwind(step, carry, shard=shard):
            late, log_adj = carry
            here = pl.ds(slot_of(shard, per_shard - 1 - step), sub)
            chance = chances[here]
            pay = pays[here]
            survive = survs[here]
            chance_adj = survive * (pay - late)
            direct = (NOTIONAL * survive) * chance / numers[here]
            annuity_adj = chance_adj * annuity_seed[here] - STRIKE * direct
            float_adj = chance_adj * float_seed[here] + direct
            level_seed[here] = annuity_adj * annuities[here] - float_adj * finals[here]
            slope_seed[here] = ACCRUAL * annuity_adj
            gained = chance * pay
            log_adj = log_adj - survive * gained
            numer_adj[here] = log_adj
            return (gained + late * (1.0 - chance), log_adj)

        late, log_adj = lax.fori_loop(0, per_shard, unwind, (late, log_adj), unroll=per_shard)
        if odd:
            here = pl.ds(slot_of(shard, per_shard), sub)
            level_seed[here] = jnp.zeros(tile, f32)
            slope_seed[here] = jnp.zeros(tile, f32)
        if shard > 0:
            log_adj = log_adj * ends[shard - 1] / mail(shard - 1, lay.numer)

    def backward_pair(shard, back, pos):
        index = pairs - 1 - back
        offset = 2 * index
        date = shard * per_shard + offset
        opening, _ = opening_pair(shard, offset)
        begin = opening // BLOCK
        horizon = horizons(date)
        slot = slot_of(shard, offset)
        level = level_seed[pl.ds(slot, 2 * sub)]
        slope = slope_seed[pl.ds(slot, 2 * sub)]
        steps = blocks - begin + 1
        first = pos - steps
        bank = (shard * pairs + index) * (blocks + 1)

        def one_block(turn, sums):
            sums = list(sums)
            step = steps - 1 - turn
            block = begin + step
            at = (first + step) * BLOCK
            spots = [(blocks - block) * sub + inner * (span * sub) for inner in range(BLOCK)]
            laters = [adjoint[pl.ds(spot, 2 * sub)] for spot in spots]
            kept = []
            for inner in reversed(range(BLOCK)):
                row = block * BLOCK + inner
                lead = res_lead[at + inner]
                old = res_old[at + inner]
                pull = (level - slope * res_sum[at + inner]) * (1.0 - res_disc[at + inner])
                inward = laters[inner] - pull
                timed = (horizon * lead) * inward
                sums[0] = sums[0] + timed
                drive_adj = sums[0]
                for f in range(1, factors):
                    scale = table(1 + f, row)
                    sums[f] = sums[f] + scale * timed
                    drive_adj = drive_adj + scale * sums[f]
                drive_adj = lead * drive_adj
                part = drive_adj * old
                kept.append(
                    (
                        inner,
                        inward + (part - part * old),
                        timed * res_tilt[at + inner] + (drive_adj - part),
                    )
                )
            for inner, earlier, _ in kept:
                adjoint[pl.ds(spots[inner], 2 * sub)] = earlier
            folded = [grad for _, _, grad in reversed(kept)]
            reach = 1
            while reach < sub:
                kept_side = (side // reach) % 2 == 0
                folded = [
                    jnp.where(
                        kept_side,
                        first_half + pltpu.roll(first_half, 2 * sub - reach, 0),
                        second_half + pltpu.roll(second_half, reach, 0),
                    )
                    for first_half, second_half in zip(folded[::2], folded[1::2])
                ]
                reach *= 2
            for index, grad in enumerate(folded):
                grads[(bank + block) * (BLOCK // sub) + index] = grad
            return tuple(sums)

        def patch(row, slot, fix):
            adjoint[pl.ds(place_of(row), sub)] = numer_adj[pl.ds(slot, sub)] * fix[pl.ds(slot, sub)]

        sums = (jnp.zeros(pair_tile, f32),) * factors
        turn = steps - 1 - ((opening + 1) // BLOCK - begin)
        sums = lax.fori_loop(0, turn, one_block, sums)

        def patch_second():
            patch(opening, slot + sub, near_fix)
            patch(opening + 1, slot + sub, last_fix)

        if odd:
            pl.when(offset + 1 < per_shard)(patch_second)
        else:
            patch_second()
        lax.fori_loop(turn, steps, one_block, sums)
        patch(jnp.maximum(opening - 2, 0), slot, near_fix)
        patch(opening - 1, slot, last_fix)
        return first

    for shard in reversed(range(shards)):
        pos = lax.fori_loop(0, pairs, functools.partial(backward_pair, shard), pos)
        if shard > 0:

            for row in range(lowest[shard], forwards):
                start = ACCRUAL * mail(shard - 1, lay.rates + row - lay.low_row)
                here = pl.ds(place_of(row), sub)
                adjoint[here] = adjoint[here] * state(rate, row, shard - 1) / start

    ones = jnp.ones((LANES, LANES), jnp.bfloat16)
    pieces = (blocks + 1) * (BLOCK // sub)
    shape = (pieces, 2 * sub, LANES)
    spread = lax.broadcasted_iota(jnp.int32, shape, 0) * sub
    spread = spread + lax.broadcasted_iota(jnp.int32, shape, 1)
    spread = jnp.where(lax.broadcasted_iota(jnp.int32, shape, 1) < sub, spread, spread - sub - BLOCK)
    on_lane = spread == lax.broadcasted_iota(jnp.int32, shape, 2)

    def along(picked):
        return jnp.dot(picked, ones, preferred_element_type=f32)

    def collect(pair, _):
        picked = grads[pl.ds(pair * pieces, pieces)].reshape(pieces * 2 * sub, LANES)
        top = picked.astype(jnp.bfloat16)
        rest = (picked - top.astype(f32)).astype(jnp.bfloat16)
        total = jnp.where(on_lane, (along(top) + along(rest)).reshape(shape), 0.0)
        total = jnp.sum(total, axis=0)
        low = jnp.sum(jnp.where(is_low, total, 0.0), axis=0, keepdims=True)
        high = jnp.sum(jnp.where(is_low, 0.0, total), axis=0, keepdims=True)
        vega_ref[pl.ds(2 * pair, 1)] = low[:, :forwards]
        vega_ref[pl.ds(2 * pair + 1, 1)] = high[:, :forwards]
        return 0

    lax.fori_loop(0, shards * pairs, collect, 0, unroll=4)


def by_source(own, received, place):
    count = len(received) + 1
    parts = [own] + received[::-1]
    doubled = jnp.concatenate(parts + parts, axis=0)
    start = lax.rem(count - place, count) * own.shape[0]
    return lax.dynamic_slice_in_dim(doubled, start, count * own.shape[0], 0)


def shifted(value, axis, step):
    count = lax.axis_size(axis)
    return lax.ppermute(value, axis, [(s, (s + step) % count) for s in range(count)])


def total_over(value, axis):
    count = lax.axis_size(axis)
    if count & (count - 1):
        return lax.psum(value, axis)
    step = 1
    while step < count:
        masks = [step]
        if step > 1 and 2 * step < count:
            masks = [step, 2 * step, 3 * step]
        heard = [lax.ppermute(value, axis, [(s, s ^ mask) for s in range(count)]) for mask in masks]
        value = value + heard[0]
        if len(heard) > 1:
            value = value + (heard[1] + heard[2])
        step *= 2 if len(masks) == 1 else 4
    return value


def local(
    start_curve,
    loadings,
    vols,
    shocks,
    exercise_bits,
    regress,
    date_slot,
    ck_rates,
    ck_numer,
    ck_survive,
):
    shards = lax.axis_size("tm")
    groups = lax.axis_size("paths")
    place = lax.axis_index("tm")
    per_shard, forwards = vols.shape
    factors, paths = shocks.shape[1:]
    lay = Layout(shards, per_shard, forwards, factors, regress.shape[1], paths)
    sub, blocks, pairs = lay.sub, lay.blocks, lay.pairs
    f32 = jnp.float32
    smem = pl.BlockSpec(memory_space=pltpu.SMEM)
    vmem = pl.BlockSpec(memory_space=pltpu.VMEM)
    spot = place.reshape(1).astype(jnp.int32)

    sources = (
        shocks,
        exercise_bits,
        ck_rates,
        ck_numer,
        ck_survive,
        vols,
        regress.T,
        date_slot.reshape(1, per_shard),
    )
    sources = tuple(pltpu.with_memory_space_constraint(source, pltpu.HBM) for source in sources)
    messages = pl.pallas_call(
        functools.partial(pack_kernel, lay=lay, count=len(sources)),
        out_shape=[jax.ShapeDtypeStruct((lay.flat, LANES), f32)] * shards,
        in_specs=[smem] + [pl.BlockSpec(memory_space=pltpu.HBM)] * len(sources),
        out_specs=[vmem] * shards,
        scratch_shapes=[pltpu.VMEM(source.shape, source.dtype) for source in sources]
        + [pltpu.SemaphoreType.DMA((len(sources),))],
        compiler_params=pltpu.CompilerParams(vmem_limit_bytes=16 * 1024 * 1024),
        name="pack",
    )(spot, *sources)
    received = [shifted(messages[step], "tm", step) for step in range(1, shards)]

    loads = loadings / jnp.sqrt(jnp.sum(loadings * loadings, axis=0, keepdims=True))
    kinds = jnp.concatenate([loads[:1], 0.5 / loads[:1], loads[1:] / loads[:1]])
    ahead = jnp.pad(kinds, ((0, 0), (0, BLOCK)), constant_values=1.0)
    behind = jnp.pad(kinds, ((0, 0), (BLOCK, 0)), constant_values=1.0)
    tables = jnp.broadcast_to(
        jnp.stack([ahead, behind], axis=-1).reshape(-1, 2, 1, 1),
        (kinds.shape[0] * (forwards + BLOCK), 2, sub, LANES),
    ).reshape(-1, 2 * sub, LANES)

    iterations = sum(
        blocks - (2 * (s * per_shard + 2 * k) + 1) // BLOCK + 1
        for s in range(shards)
        for k in range(pairs)
    )
    residual = pltpu.VMEM((iterations * BLOCK, 2 * sub, LANES), f32)
    per_slot = pltpu.VMEM((shards * 2 * pairs * sub, LANES), f32)
    state_rows = BLOCK * (blocks + 2) * sub
    vega_part, value_part = pl.pallas_call(
        functools.partial(sweep_kernel, lay=lay),
        out_shape=(
            jax.ShapeDtypeStruct((shards * 2 * pairs, forwards), f32),
            jax.ShapeDtypeStruct((sub, LANES), f32),
        ),
        in_specs=[smem, smem, vmem] + [pl.BlockSpec(memory_space=pl.ANY)] * shards,
        out_specs=(vmem, vmem),
        scratch_shapes=[
            pltpu.VMEM((shards, lay.flat, LANES), f32),
            pltpu.SMEM((shards * lay.small_rows * LANES,), f32),
            pltpu.VMEM((shards * state_rows, LANES), f32),
            pltpu.VMEM((state_rows, LANES), f32),
            residual,
            residual,
            residual,
            residual,
            residual,
            pltpu.VMEM((shards * pairs * (blocks + 1) * (BLOCK // sub), 2 * sub, LANES), f32),
        ]
        + [per_slot] * 13
        + [
            pltpu.VMEM((state_rows, LANES), f32),
            pltpu.SemaphoreType.DMA((shards,)),
            pltpu.SemaphoreType.DMA((shards, lay.small_rows)),
        ],
        compiler_params=pltpu.CompilerParams(vmem_limit_bytes=48 * 1024 * 1024),
        name="sweep",
    )(spot, start_curve, tables, messages[0], *received)

    parts = vega_part.reshape(shards, 2 * pairs, forwards)[:, :per_shard].reshape(shards, -1)
    cut = per_shard * forwards
    tail = jnp.broadcast_to(value_part.reshape(1, -1), (shards, lay.per_device))
    message = jnp.concatenate([parts, tail], axis=1)
    mine = lax.dynamic_index_in_dim(message, place, 0, keepdims=False)
    others = []
    for step in range(1, shards):
        sent = lax.dynamic_index_in_dim(message, lax.rem(place + step, shards), 0, keepdims=False)
        others.append(shifted(sent, "tm", step))
    path_value = by_source(
        mine[cut:].reshape(1, -1), [part[cut:].reshape(1, -1) for part in others], place
    ).reshape(-1)
    summed = mine[:cut]
    for part in others:
        summed = summed + part[:cut]
    summed = total_over(summed.reshape(per_shard, forwards), "paths")
    date = place * per_shard + jnp.arange(per_shard, dtype=jnp.int32)
    alive = jnp.arange(forwards, dtype=jnp.int32)[None, :] >= 2 * date[:, None] + 1
    weight = NOTIONAL / (paths * groups)
    vega = jnp.where(alive, summed * (weight / vols), 0.0)
    return (vega, path_value)


def solution(mesh):
    return jax.shard_map(
        local,
        mesh=mesh,
        in_specs=(
            P(),
            P(),
            P("tm", None),
            P("tm", None, "paths"),
            P("tm", "paths"),
            P("tm", None),
            P("tm"),
            P("tm", None, "paths"),
            P("tm", "paths"),
            P("tm", "paths"),
        ),
        out_specs=(P("tm", None), P("paths")),
        check_vma=False,
    )
```

```python
import functools

import jax
import jax.numpy as jnp
from jax import lax
from jax.experimental import pallas as pl
from jax.experimental.pallas import tpu as pltpu
from jax.sharding import PartitionSpec as P

ACCRUAL = 0.25
STRIKE = 0.04
SMOOTHING = 0.01
NOTIONAL = 100.0
LANES = 128
BLOCK = 8
LOG2E = 1.4426950408889634


class Layout:
    def __init__(self, shards, per_shard, forwards, factors, basis, paths):
        self.shards = shards
        self.per_shard = per_shard
        self.forwards = forwards
        self.factors = factors
        self.basis = basis
        self.per_device = paths // shards
        self.sub = self.per_device // LANES
        self.pairs = -(-per_shard // 2)
        self.low_row = max(0, 2 * per_shard - 1)
        self.shock = 0
        self.flag = self.shock + 2 * self.pairs * factors
        self.rates = self.flag + 2 * self.pairs
        self.numer = self.rates + forwards - self.low_row
        self.survive = self.numer + 1
        small = self.survive + 1
        while (small * self.sub) % 8:
            small += 1
        self.small = small * self.sub
        self.regress_at = per_shard
        self.slot_at = per_shard + basis
        self.small_rows = per_shard + basis + 1
        total = -(-(self.small + self.small_rows) // 8) * 8
        self.flat = total
        self.blocks = forwards // BLOCK


def pack_kernel(place_ref, *refs, lay, count):
    sources = refs[:count]
    out_refs = refs[count : count + lay.shards]
    held = refs[count + lay.shards : 2 * count + lay.shards]
    arrived = refs[-1]
    copies = [
        pltpu.make_async_copy(source, target, arrived.at[index])
        for index, (source, target) in enumerate(zip(sources, held))
    ]
    for copy in copies:
        copy.start()
    for copy in copies:
        copy.wait()
    shock_ref, flag_ref, rate_ref, numer_ref, survive_ref, vol_ref, regress_ref, slot_ref = held
    place = place_ref[0]
    sub = lay.sub
    for step, out in enumerate(out_refs):
        target = lax.rem(place + step, lay.shards)
        for q in range(sub):
            lanes = pl.ds(pl.multiple_of(target * lay.per_device + q * LANES, LANES), LANES)
            for d in range(lay.per_shard):
                row = lay.shock + (d // 2) * lay.factors * 2 + d % 2
                out[pl.ds(row * sub + q, lay.factors, stride=2 * sub), :] = shock_ref[d, :, lanes]
            out[pl.ds(lay.flag * sub + q, lay.per_shard, stride=sub), :] = flag_ref[
                :, lanes
            ].astype(jnp.float32)
            out[
                pl.ds(lay.rates * sub + q, lay.forwards - lay.low_row, stride=sub), :
            ] = rate_ref[0, lay.low_row :, lanes]
            out[pl.ds(lay.numer * sub + q, 1), :] = numer_ref[:, lanes]
            out[pl.ds(lay.survive * sub + q, 1), :] = survive_ref[:, lanes]
        base = lay.small
        out[pl.ds(base, lay.per_shard), :] = jnp.zeros((lay.per_shard, LANES), jnp.float32)
        out[pl.ds(base, lay.per_shard), 0 : lay.forwards] = vol_ref[...]
        out[pl.ds(base + lay.regress_at, lay.basis), 0 : lay.per_shard] = regress_ref[...]
        out[pl.ds(base + lay.slot_at, 1), 0 : lay.per_shard] = slot_ref[...].astype(jnp.float32)


def sweep_kernel(place_ref, curve_ref, table_ref, *refs, lay):
    shards, per_shard, forwards = lay.shards, lay.per_shard, lay.forwards
    factors, basis, sub, blocks, pairs = lay.factors, lay.basis, lay.sub, lay.blocks, lay.pairs
    block_refs = refs[:shards]
    vega_ref, value_ref = refs[shards : shards + 2]
    (
        inbox,
        smalls,
        rate,
        disc,
        res_old,
        res_disc,
        res_tilt,
        res_sum,
        res_lead,
        grads,
        annuities,
        finals,
        numers,
        near_fix,
        last_fix,
        float_seed,
        annuity_seed,
        level_seed,
        slope_seed,
        numer_adj,
        survs,
        chances,
        pays,
        adjoint,
        arrived,
        small_arrived,
    ) = refs[shards + 2 :]
    f32 = jnp.float32
    tile = (sub, LANES)
    pair_tile = (2 * sub, LANES)
    place = place_ref[0]
    odd = per_shard % 2
    span = blocks + 2
    state_rows = BLOCK * span * sub
    lowest = [max(0, 2 * s * per_shard - 1) for s in range(shards)]
    side = lax.broadcasted_iota(jnp.int32, pair_tile, 0)
    is_low = side < sub

    def fetch(step, source):
        return pltpu.make_async_copy(block_refs[step], inbox.at[source], arrived.at[source])

    def fetch_small(step, source, row):
        spot = (source * lay.small_rows + row) * LANES
        return pltpu.make_async_copy(
            block_refs[step].at[lay.small + row],
            smalls.at[pl.ds(pl.multiple_of(spot, LANES), LANES)],
            small_arrived.at[source, row],
        )

    for step in range(shards):
        source = lax.rem(place - step + shards, shards)
        for row in range(lay.small_rows):
            fetch_small(step, source, row).start()
    for step in range(shards):
        fetch(step, lax.rem(place - step + shards, shards)).start()

    def await_source(shard):
        for row in range(lay.small_rows):
            fetch_small(0, shard, row).wait()
        fetch(0, shard).wait()

    def clear(ref):
        rows = ref.shape[0]

        def one(row, _):
            ref[pl.ds(pl.multiple_of(row * 8, 8), 8)] = jnp.zeros((8, LANES), f32)
            return 0

        lax.fori_loop(0, rows // 8, one, 0, unroll=8)

    clear(rate)
    clear(disc)
    clear(adjoint)

    def mail(shard, row, count=1):
        return inbox[shard, pl.ds(row * sub, count * sub)]

    def place_of(row):
        if isinstance(row, int):
            return (row % BLOCK * span + blocks - row // BLOCK) * sub
        return (lax.rem(row, BLOCK) * span + blocks - lax.div(row, BLOCK)) * sub

    def state(ref, row, shard=0):
        return ref[pl.ds(shard * state_rows + place_of(row), sub)]

    def slot_of(shard, offset):
        return (shard * 2 * pairs + offset) * sub

    def both(low, high):
        return jnp.where(is_low, low, high)

    def horizons(date):
        return both(jnp.where(date == 0, ACCRUAL, 2.0 * ACCRUAL), 2.0 * ACCRUAL)

    def opening_pair(shard, offset):
        opening = 2 * (shard * per_shard + offset) + 1
        second = opening + 2
        if odd:
            second = jnp.where(offset + 1 < per_shard, second, 4 * forwards)
        return opening, second

    def volatility(shard, offset, block, reach):
        base = (shard * lay.small_rows + offset) * LANES + block * BLOCK
        beyond = block * BLOCK - reach
        found = []
        for inner in range(BLOCK):
            raw = both(smalls[base + inner], smalls[base + (LANES - BLOCK + inner)])
            found.append(jnp.where(beyond >= -inner, raw, 0.0))
        return found

    def table(kind, row):
        return table_ref[kind * (forwards + BLOCK) + row]

    def forward_pair(shard, index, carry):
        pos, numer = carry
        offset = 2 * index
        date = shard * per_shard + offset
        opening, second = opening_pair(shard, offset)
        reach = both(opening, second + BLOCK)
        begin = opening // BLOCK
        horizon = horizons(date)
        timer = horizon * LOG2E
        root = both(jnp.where(date == 0, ACCRUAL**-0.5, (2.0 * ACCRUAL) ** -0.5), (2.0 * ACCRUAL) ** -0.5)
        sums = tuple(
            mail(shard, lay.shock + (index * factors + f) * 2, 2) * root for f in range(factors)
        )

        if odd:
            real = is_low | (offset + 1 < per_shard)
            sums = tuple(jnp.where(real, part, 0.0) for part in sums)

        def one_block(step, held):
            sums, bond, total = held
            sums = list(sums)
            block = begin + step
            at = (pos + step) * BLOCK
            spots = [(blocks - block) * sub + inner * (span * sub) for inner in range(BLOCK)]
            sigmas = volatility(shard, offset, block, reach)
            rates = [rate[pl.ds(shard * state_rows + spot, 2 * sub)] for spot in spots]
            olds = [disc[pl.ds(spot, 2 * sub)] for spot in spots]
            kept = []
            for inner in range(BLOCK):
                row = block * BLOCK + inner
                sigma = sigmas[inner]
                lead = sigma * table(0, row)
                half = sigma * table(1, row)
                drive = lead - lead * olds[inner]
                sums[0] = sums[0] + drive
                tilt = sums[0]
                for f in range(1, factors):
                    scale = table(1 + f, row)
                    sums[f] = sums[f] + scale * drive
                    tilt = tilt + scale * sums[f]
                tilt = tilt - half
                new = rates[inner] * jnp.exp2((timer * lead) * tilt)
                fresh = 1.0 / (1.0 + new)
                alive = sigma > 0.0
                shown = jnp.where(alive, fresh, 1.0)
                kept.append((new, fresh, shown, tilt - half, total, lead))
                bond = bond * shown
                total = total + jnp.where(alive, bond, 0.0)
            for inner, (new, fresh, shown, lean, before, lead) in enumerate(kept):
                rate[pl.ds(shard * state_rows + spots[inner], 2 * sub)] = new
                disc[pl.ds(spots[inner], 2 * sub)] = fresh
                res_old[at + inner] = olds[inner]
                res_disc[at + inner] = shown
                res_tilt[at + inner] = lean
                res_sum[at + inner] = before
                res_lead[at + inner] = lead
            return (tuple(sums), bond, total)

        steps = blocks - begin + 1
        _, bond, total = lax.fori_loop(
            0, steps, one_block, (sums, jnp.ones(pair_tile, f32), jnp.zeros(pair_tile, f32))
        )
        slot = slot_of(shard, offset)
        annuities[pl.ds(slot, 2 * sub)] = ACCRUAL * total
        finals[pl.ds(slot, 2 * sub)] = bond
        near = jnp.maximum(opening - 2, 0)
        numer = numer * (1.0 + state(rate, opening - 1, shard))
        numer = numer * jnp.where(date == 0, 1.0, 1.0 + state(rate, near, shard))
        numers[pl.ds(slot, sub)] = numer
        later = numer * (1.0 + state(rate, opening, shard)) * (
            1.0 + state(rate, opening + 1, shard)
        )
        if odd:
            later = jnp.where(offset + 1 < per_shard, later, numer)
        numers[pl.ds(slot + sub, sub)] = later
        near_fix[pl.ds(slot, sub)] = 1.0 - state(disc, near)
        last_fix[pl.ds(slot, sub)] = 1.0 - state(disc, opening - 1)
        near_fix[pl.ds(slot + sub, sub)] = 1.0 - state(disc, opening)
        last_fix[pl.ds(slot + sub, sub)] = 1.0 - state(disc, opening + 1)
        return (pos + steps, later)

    pos = jnp.int32(0)
    ends = []
    for shard in range(shards):
        await_source(shard)
        for row in range(lowest[shard], forwards):
            if shard == 0:
                start = jnp.full(tile, ACCRUAL * curve_ref[row], f32)
            else:
                start = ACCRUAL * mail(shard - 1, lay.rates + row - lay.low_row)
            rate[pl.ds(shard * state_rows + place_of(row), sub)] = start
            disc[pl.ds(place_of(row), sub)] = 1.0 / (1.0 + start)
        numer = jnp.ones(tile, f32) if shard == 0 else mail(shard - 1, lay.numer)
        pos, numer = lax.fori_loop(
            0, pairs, functools.partial(forward_pair, shard), (pos, numer)
        )
        ends.append(numer)

    value = jnp.zeros(tile, f32)
    for shard in range(shards):

        def stage(index, _, shard=shard):
            offset = 2 * index
            slot = slot_of(shard, offset)
            pair = pl.ds(slot, 2 * sub)
            annuity = annuities[pair]
            floating = 1.0 - finals[pair]
            marks = []
            for step in range(2):
                spot = jnp.minimum(offset + step, per_shard - 1)
                named = smalls[(shard * lay.small_rows + lay.slot_at) * LANES + spot]
                named = named.astype(jnp.int32)
                owner = lax.div(named, per_shard)
                base = (owner * lay.small_rows + lay.regress_at) * LANES
                base = base + lax.rem(named, per_shard)
                marks.append([smalls[base + q * LANES] for q in range(basis)])
            w = [both(marks[0][q], marks[1][q]) for q in range(basis)]
            if odd:
                real = is_low | (offset + 1 < per_shard)
                annuity = jnp.where(real, annuity, 1.0)
            inverse = 1.0 / annuity
            swap = floating * inverse
            money = (swap - STRIKE) * (1.0 / SMOOTHING)
            exercise = floating - STRIKE * annuity
            inner = w[3] + money * (w[4] + money * w[5])
            continuation = w[0] + money * (w[1] + money * w[2]) + annuity * inner
            sigmoid = jax.nn.sigmoid((exercise - continuation) * (1.0 / SMOOTHING))
            flag = mail(shard, lay.flag + offset, 2)
            if odd:
                flag = jnp.where(real, flag, 0.0)
            chance = flag * sigmoid
            slope = chance * (1.0 - sigmoid) * (1.0 / SMOOTHING)
            money_adj = (
                w[1] + 2.0 * (w[2] * money) + annuity * (w[4] + 2.0 * (w[5] * money))
            ) * (1.0 / SMOOTHING)
            tilt_money = money_adj * inverse
            annuity_seed[pair] = slope * (-STRIKE - inner + tilt_money * swap)
            float_seed[pair] = slope * (1.0 - tilt_money)
            chances[pair] = chance
            pays[pair] = NOTIONAL * exercise / numers[pair]
            return 0

        lax.fori_loop(0, pairs, stage, 0, unroll=pairs)
        survive = jnp.ones(tile, f32) if shard == 0 else mail(shard - 1, lay.survive)

        def gain(offset, carry, shard=shard):
            survive, value = carry
            here = pl.ds(slot_of(shard, offset), sub)
            chance = chances[here]
            survs[here] = survive
            return (survive * (1.0 - chance), value + survive * chance * pays[here])

        survive, value = lax.fori_loop(0, per_shard, gain, (survive, value), unroll=per_shard)
    value_ref[...] = value

    late = jnp.zeros(tile, f32)
    log_adj = jnp.zeros(tile, f32)
    for shard in reversed(range(shards)):

        def unwind(step, carry, shard=shard):
            late, log_adj = carry
            here = pl.ds(slot_of(shard, per_shard - 1 - step), sub)
            chance = chances[here]
            pay = pays[here]
            survive = survs[here]
            chance_adj = survive * (pay - late)
            direct = (NOTIONAL * survive) * chance / numers[here]
            annuity_adj = chance_adj * annuity_seed[here] - STRIKE * direct
            float_adj = chance_adj * float_seed[here] + direct
            level_seed[here] = annuity_adj * annuities[here] - float_adj * finals[here]
            slope_seed[here] = ACCRUAL * annuity_adj
            gained = chance * pay
            log_adj = log_adj - survive * gained
            numer_adj[here] = log_adj
            return (gained + late * (1.0 - chance), log_adj)

        late, log_adj = lax.fori_loop(0, per_shard, unwind, (late, log_adj), unroll=per_shard)
        if odd:
            here = pl.ds(slot_of(shard, per_shard), sub)
            level_seed[here] = jnp.zeros(tile, f32)
            slope_seed[here] = jnp.zeros(tile, f32)
        if shard > 0:
            log_adj = log_adj * ends[shard - 1] / mail(shard - 1, lay.numer)

    def backward_pair(shard, back, pos):
        index = pairs - 1 - back
        offset = 2 * index
        date = shard * per_shard + offset
        opening, _ = opening_pair(shard, offset)
        begin = opening // BLOCK
        horizon = horizons(date)
        slot = slot_of(shard, offset)
        level = level_seed[pl.ds(slot, 2 * sub)]
        slope = slope_seed[pl.ds(slot, 2 * sub)]
        steps = blocks - begin + 1
        first = pos - steps
        bank = (shard * pairs + index) * (blocks + 1)

        def one_block(turn, sums):
            sums = list(sums)
            step = steps - 1 - turn
            block = begin + step
            at = (first + step) * BLOCK
            spots = [(blocks - block) * sub + inner * (span * sub) for inner in range(BLOCK)]
            laters = [adjoint[pl.ds(spot, 2 * sub)] for spot in spots]
            kept = []
            for inner in reversed(range(BLOCK)):
                row = block * BLOCK + inner
                lead = res_lead[at + inner]
                old = res_old[at + inner]
                pull = (level - slope * res_sum[at + inner]) * (1.0 - res_disc[at + inner])
                inward = laters[inner] - pull
                timed = (horizon * lead) * inward
                sums[0] = sums[0] + timed
                drive_adj = sums[0]
                for f in range(1, factors):
                    scale = table(1 + f, row)
                    sums[f] = sums[f] + scale * timed
                    drive_adj = drive_adj + scale * sums[f]
                drive_adj = lead * drive_adj
                part = drive_adj * old
                kept.append(
                    (
                        inner,
                        inward + (part - part * old),
                        timed * res_tilt[at + inner] + (drive_adj - part),
                    )
                )
            for inner, earlier, _ in kept:
                adjoint[pl.ds(spots[inner], 2 * sub)] = earlier
            folded = [grad for _, _, grad in reversed(kept)]
            reach = 1
            while reach < sub:
                kept_side = (side // reach) % 2 == 0
                folded = [
                    jnp.where(
                        kept_side,
                        first_half + pltpu.roll(first_half, 2 * sub - reach, 0),
                        second_half + pltpu.roll(second_half, reach, 0),
                    )
                    for first_half, second_half in zip(folded[::2], folded[1::2])
                ]
                reach *= 2
            for index, grad in enumerate(folded):
                grads[(bank + block) * (BLOCK // sub) + index] = grad
            return tuple(sums)

        def patch(row, slot, fix):
            adjoint[pl.ds(place_of(row), sub)] = numer_adj[pl.ds(slot, sub)] * fix[pl.ds(slot, sub)]

        sums = (jnp.zeros(pair_tile, f32),) * factors
        turn = steps - 1 - ((opening + 1) // BLOCK - begin)
        sums = lax.fori_loop(0, turn, one_block, sums)

        def patch_second():
            patch(opening, slot + sub, near_fix)
            patch(opening + 1, slot + sub, last_fix)

        if odd:
            pl.when(offset + 1 < per_shard)(patch_second)
        else:
            patch_second()
        lax.fori_loop(turn, steps, one_block, sums)
        patch(jnp.maximum(opening - 2, 0), slot, near_fix)
        patch(opening - 1, slot, last_fix)
        return first

    for shard in reversed(range(shards)):
        pos = lax.fori_loop(0, pairs, functools.partial(backward_pair, shard), pos)
        if shard > 0:

            for row in range(lowest[shard], forwards):
                start = ACCRUAL * mail(shard - 1, lay.rates + row - lay.low_row)
                here = pl.ds(place_of(row), sub)
                adjoint[here] = adjoint[here] * state(rate, row, shard - 1) / start

    ones = jnp.ones((LANES, LANES), jnp.bfloat16)
    pieces = (blocks + 1) * (BLOCK // sub)
    shape = (pieces, 2 * sub, LANES)
    spread = lax.broadcasted_iota(jnp.int32, shape, 0) * sub
    spread = spread + lax.broadcasted_iota(jnp.int32, shape, 1)
    spread = jnp.where(lax.broadcasted_iota(jnp.int32, shape, 1) < sub, spread, spread - sub - BLOCK)
    on_lane = spread == lax.broadcasted_iota(jnp.int32, shape, 2)

    def along(picked):
        return jnp.dot(picked, ones, preferred_element_type=f32)

    def collect(pair, _):
        picked = grads[pl.ds(pair * pieces, pieces)].reshape(pieces * 2 * sub, LANES)
        top = picked.astype(jnp.bfloat16)
        rest = (picked - top.astype(f32)).astype(jnp.bfloat16)
        total = jnp.where(on_lane, (along(top) + along(rest)).reshape(shape), 0.0)
        total = jnp.sum(total, axis=0)
        low = jnp.sum(jnp.where(is_low, total, 0.0), axis=0, keepdims=True)
        high = jnp.sum(jnp.where(is_low, 0.0, total), axis=0, keepdims=True)
        vega_ref[pl.ds(2 * pair, 1)] = low[:, :forwards]
        vega_ref[pl.ds(2 * pair + 1, 1)] = high[:, :forwards]
        return 0

    lax.fori_loop(0, shards * pairs, collect, 0, unroll=4)


def by_source(own, received, place):
    count = len(received) + 1
    parts = [own] + received[::-1]
    doubled = jnp.concatenate(parts + parts, axis=0)
    start = lax.rem(count - place, count) * own.shape[0]
    return lax.dynamic_slice_in_dim(doubled, start, count * own.shape[0], 0)


def shifted(value, axis, step):
    count = lax.axis_size(axis)
    return lax.ppermute(value, axis, [(s, (s + step) % count) for s in range(count)])


def total_over(value, axis):
    count = lax.axis_size(axis)
    if count & (count - 1):
        return lax.psum(value, axis)
    step = 1
    while step < count:
        masks = [step]
        if step > 1 and 2 * step < count:
            masks = [step, 2 * step, 3 * step]
        heard = [lax.ppermute(value, axis, [(s, s ^ mask) for s in range(count)]) for mask in masks]
        value = value + heard[0]
        if len(heard) > 1:
            value = value + (heard[1] + heard[2])
        step *= 2 if len(masks) == 1 else 4
    return value


def local(
    start_curve,
    loadings,
    vols,
    shocks,
    exercise_bits,
    regress,
    date_slot,
    ck_rates,
    ck_numer,
    ck_survive,
):
    shards = lax.axis_size("tm")
    groups = lax.axis_size("paths")
    place = lax.axis_index("tm")
    per_shard, forwards = vols.shape
    factors, paths = shocks.shape[1:]
    lay = Layout(shards, per_shard, forwards, factors, regress.shape[1], paths)
    sub, blocks, pairs = lay.sub, lay.blocks, lay.pairs
    f32 = jnp.float32
    smem = pl.BlockSpec(memory_space=pltpu.SMEM)
    vmem = pl.BlockSpec(memory_space=pltpu.VMEM)
    spot = place.reshape(1).astype(jnp.int32)

    sources = (
        shocks,
        exercise_bits,
        ck_rates,
        ck_numer,
        ck_survive,
        vols,
        regress.T,
        date_slot.reshape(1, per_shard),
    )
    sources = tuple(pltpu.with_memory_space_constraint(source, pltpu.HBM) for source in sources)
    messages = pl.pallas_call(
        functools.partial(pack_kernel, lay=lay, count=len(sources)),
        out_shape=[jax.ShapeDtypeStruct((lay.flat, LANES), f32)] * shards,
        in_specs=[smem] + [pl.BlockSpec(memory_space=pltpu.HBM)] * len(sources),
        out_specs=[vmem] * shards,
        scratch_shapes=[pltpu.VMEM(source.shape, source.dtype) for source in sources]
        + [pltpu.SemaphoreType.DMA((len(sources),))],
        compiler_params=pltpu.CompilerParams(vmem_limit_bytes=16 * 1024 * 1024),
        name="pack",
    )(spot, *sources)
    sent_by = {}
    for step in reversed(range(1, shards)):
        sent_by[step] = shifted(messages[step], "tm", step)
    received = [sent_by[step] for step in range(1, shards)]

    loads = loadings / jnp.sqrt(jnp.sum(loadings * loadings, axis=0, keepdims=True))
    kinds = jnp.concatenate([loads[:1], 0.5 / loads[:1], loads[1:] / loads[:1]])
    ahead = jnp.pad(kinds, ((0, 0), (0, BLOCK)), constant_values=1.0)
    behind = jnp.pad(kinds, ((0, 0), (BLOCK, 0)), constant_values=1.0)
    tables = jnp.broadcast_to(
        jnp.stack([ahead, behind], axis=-1).reshape(-1, 2, 1, 1),
        (kinds.shape[0] * (forwards + BLOCK), 2, sub, LANES),
    ).reshape(-1, 2 * sub, LANES)

    iterations = sum(
        blocks - (2 * (s * per_shard + 2 * k) + 1) // BLOCK + 1
        for s in range(shards)
        for k in range(pairs)
    )
    residual = pltpu.VMEM((iterations * BLOCK, 2 * sub, LANES), f32)
    per_slot = pltpu.VMEM((shards * 2 * pairs * sub, LANES), f32)
    state_rows = BLOCK * (blocks + 2) * sub
    vega_part, value_part = pl.pallas_call(
        functools.partial(sweep_kernel, lay=lay),
        out_shape=(
            jax.ShapeDtypeStruct((shards * 2 * pairs, forwards), f32),
            jax.ShapeDtypeStruct((sub, LANES), f32),
        ),
        in_specs=[smem, smem, vmem] + [pl.BlockSpec(memory_space=pl.ANY)] * shards,
        out_specs=(vmem, vmem),
        scratch_shapes=[
            pltpu.VMEM((shards, lay.flat, LANES), f32),
            pltpu.SMEM((shards * lay.small_rows * LANES,), f32),
            pltpu.VMEM((shards * state_rows, LANES), f32),
            pltpu.VMEM((state_rows, LANES), f32),
            residual,
            residual,
            residual,
            residual,
            residual,
            pltpu.VMEM((shards * pairs * (blocks + 1) * (BLOCK // sub), 2 * sub, LANES), f32),
        ]
        + [per_slot] * 13
        + [
            pltpu.VMEM((state_rows, LANES), f32),
            pltpu.SemaphoreType.DMA((shards,)),
            pltpu.SemaphoreType.DMA((shards, lay.small_rows)),
        ],
        compiler_params=pltpu.CompilerParams(vmem_limit_bytes=48 * 1024 * 1024),
        name="sweep",
    )(spot, start_curve, tables, messages[0], *received)

    parts = vega_part.reshape(shards, 2 * pairs, forwards)[:, :per_shard].reshape(shards, -1)
    cut = per_shard * forwards
    tail = jnp.broadcast_to(value_part.reshape(1, -1), (shards, lay.per_device))
    message = jnp.concatenate([parts, tail], axis=1)
    mine = lax.dynamic_index_in_dim(message, place, 0, keepdims=False)
    others = []
    for step in range(1, shards):
        sent = lax.dynamic_index_in_dim(message, lax.rem(place + step, shards), 0, keepdims=False)
        others.append(shifted(sent, "tm", step))
    path_value = by_source(
        mine[cut:].reshape(1, -1), [part[cut:].reshape(1, -1) for part in others], place
    ).reshape(-1)
    summed = mine[:cut]
    for part in others:
        summed = summed + part[:cut]
    summed = total_over(summed.reshape(per_shard, forwards), "paths")
    date = place * per_shard + jnp.arange(per_shard, dtype=jnp.int32)
    alive = jnp.arange(forwards, dtype=jnp.int32)[None, :] >= 2 * date[:, None] + 1
    weight = NOTIONAL / (paths * groups)
    vega = jnp.where(alive, summed * (weight / vols), 0.0)
    return (vega, path_value)


def solution(mesh):
    return jax.shard_map(
        local,
        mesh=mesh,
        in_specs=(
            P(),
            P(),
            P("tm", None),
            P("tm", None, "paths"),
            P("tm", "paths"),
            P("tm", None),
            P("tm"),
            P("tm", None, "paths"),
            P("tm", "paths"),
            P("tm", "paths"),
        ),
        out_specs=(P("tm", None), P("paths")),
        check_vma=False,
    )
```
